32 devices in a mesh: seq: 4 (over y, core), head: 8 (over z, x).
Axes of the slice: x: 2, y: 2, z: 4, core: 2. Of those that a mesh axis runs over, the one named last changes fastest.
Arguments:
- tokens: bfloat16 [3072, 8192], P('seq', 'head'), may hold values from -6 to 6
- w_query: bfloat16 [8192, 8192], P(None, 'head'), may hold values from -0.0625 to 0.0625
- w_key: bfloat16 [8192, 1024], P(None, 'head'), may hold values from -0.0625 to 0.0625
- w_value: bfloat16 [8192, 1024], P(None, 'head'), may hold values from -0.0625 to 0.0625
- map_query: float32 [64, 128, 64], P('head'), may hold values from -0.5 to 0.5
- map_key: float32 [64, 128, 64], P('head'), may hold values from -0.5 to 0.5
Outputs:
- student_out: bfloat16 [3072, 8192], P('seq', 'head')
- grad_query_map: float32 [64, 128, 64], P('head')
- grad_key_map: float32 [64, 128, 64], P('head')
The draws below stay inside these ranges and needn't reach their ends.
All inputs are finite; a program needn't handle non-finite values.
Results may differ from the reference program's by a relative error of at most 0.013.
Values may be sent and summed in bfloat16 or wider, within the bound.
A program may use at most 128 MiB of HBM per device.

```python
import math
import jax
import jax.numpy as jnp
from jax import lax

D = 8192
HEADS = 64
KVH = 8
DH = 128
FEAT = 64
TOKENS = 3072


def block_levels(rng, shape, shards, smallest, largest):
    factor_of = 1.0
    for position, blocks in shards:
        heights = jax.random.uniform(jax.random.fold_in(jax.random.fold_in(rng, 6), position), (blocks,), jnp.float32, smallest / len(shards), largest / len(shards))
        factor_of = factor_of * jnp.repeat(jnp.exp(heights), shape[position] // blocks).reshape((-1,) + (1,) * (len(shape) - 1 - position))
    return factor_of


def gaussian(key, dims, deviation, limit, shards=(), held_as=jnp.bfloat16):
    loudness = block_levels(key, dims, shards, -0.22, 0.18) if shards else 1.0
    entries = jax.random.normal(key, dims, jnp.float32) * deviation * loudness
    return jnp.minimum(jnp.maximum(entries, -limit), limit).astype(held_as)


def setup_inputs(seed: int = 0) -> dict:
    seeds = jax.random.split(jax.random.key(seed), 7)
    tokens = gaussian(seeds[0], (TOKENS, D), 1.0, 6.0, ((0, 4), (1, 8)))
    w_query = gaussian(seeds[1], (D, HEADS * DH), D ** -0.5, 0.0625, ((1, 8),))
    w_key = gaussian(seeds[2], (D, KVH * DH), D ** -0.5, 0.0625, ((1, 8),))
    w_value = gaussian(seeds[3], (D, KVH * DH), D ** -0.5, 0.0625, ((1, 8),))
    map_query = gaussian(seeds[4], (HEADS, DH, FEAT), DH ** -0.5, 0.5, ((0, 8),), jnp.float32)
    map_key = gaussian(seeds[5], (HEADS, DH, FEAT), DH ** -0.5, 0.5, ((0, 8),), jnp.float32)
    return dict(tokens=tokens, w_query=w_query, w_key=w_key, w_value=w_value, map_query=map_query, map_key=map_key)


ROPE_BASE = 500000.0
MATMUL_ACCURACY = lax.Precision.HIGHEST

def rope_tables(length, width, offset):
    half_width = width // 2
    positions = (offset + jnp.arange(length)).astype(jnp.float32)
    exponent = jnp.arange(half_width).astype(jnp.float32) * (2.0 / width)
    frequency = jnp.power(jnp.float32(ROPE_BASE), -exponent)
    angles = positions[:, None] * frequency[None, :]
    return (jnp.cos(angles), jnp.sin(angles))

def rotate(vectors, cosine, sine):
    half_width = vectors.shape[-1] // 2
    first = vectors[..., :half_width]
    second = vectors[..., half_width:]
    cosine = cosine[:, None, :]
    sine = sine[:, None, :]
    return jnp.concatenate([first * cosine - second * sine, second * cosine + first * sine], axis=-1)

def feature_map(vectors, weights):
    logits = jnp.einsum('thd,hdf->thf', vectors, weights, precision=MATMUL_ACCURACY)
    upper = jnp.exp(logits)
    lower = jnp.exp(-logits)
    return jnp.concatenate([upper / lax.optimization_barrier(jnp.sum(upper, -1, keepdims=True)), lower / lax.optimization_barrier(jnp.sum(lower, -1, keepdims=True))], axis=-1)

def reference(tokens, w_query, w_key, w_value, map_query, map_key):
    length = tokens.shape[0]
    group = HEADS // KVH
    query_rows = jnp.dot(tokens, w_query, preferred_element_type=jnp.float32).reshape(length, HEADS, DH)
    keys = jnp.dot(tokens, w_key, preferred_element_type=jnp.float32).astype(jnp.bfloat16)
    values = jnp.dot(tokens, w_value, preferred_element_type=jnp.float32).astype(jnp.bfloat16)
    cosine, sine = rope_tables(length, DH, 0)
    queries_rot = rotate(query_rows, cosine, sine).astype(jnp.bfloat16)
    keys_rot = rotate(keys.astype(jnp.float32).reshape(length, KVH, DH), cosine, sine).astype(jnp.bfloat16)
    values = values.reshape(length, KVH, DH)
    causal = jnp.arange(length)[None, :] <= jnp.arange(length)[:, None]
    query_head_count = jnp.transpose(queries_rot, (1, 0, 2))
    key_heads = jnp.transpose(keys_rot, (1, 0, 2))
    value_heads = jnp.transpose(values, (1, 0, 2))
    scale = 1.0 / math.sqrt(DH)

    def teacher_head(index):
        shared_index = index // group
        scores = jnp.dot(query_head_count[index], key_heads[shared_index].T, preferred_element_type=jnp.float32) * scale
        weights = jnp.exp(jnp.where(causal, scores, -1e+30))
        total = lax.optimization_barrier(jnp.sum(weights, -1))
        mixed = jnp.dot(weights.astype(jnp.bfloat16), value_heads[shared_index], preferred_element_type=jnp.float32)
        return (mixed / total[:, None]).astype(jnp.bfloat16)
    teacher = lax.map(teacher_head, jnp.arange(HEADS))
    target = jnp.transpose(teacher, (1, 0, 2)).astype(jnp.float32)
    keys_wide = jnp.repeat(keys_rot.astype(jnp.float32), group, axis=1)
    value_rows_broad = jnp.transpose(jnp.repeat(values.astype(jnp.float32), group, axis=1), (1, 0, 2))
    query_float = queries_rot.astype(jnp.float32)
    mask = causal.astype(jnp.float32)

    def student_head(inputs):
        query_feature_rows, key_feature_rows, head_values = inputs
        within = jnp.dot(query_feature_rows, key_feature_rows.T, precision=MATMUL_ACCURACY) * mask
        numerator = jnp.dot(within, head_values, precision=MATMUL_ACCURACY)
        return numerator / lax.optimization_barrier(jnp.sum(within, -1))[:, None]

    def student(query_weights, key_weights):
        query_features = jnp.transpose(feature_map(query_float, query_weights), (1, 0, 2))
        key_features = jnp.transpose(feature_map(keys_wide, key_weights), (1, 0, 2))
        outputs = lax.map(jax.checkpoint(student_head), (query_features, key_features, value_rows_broad))
        outputs = jnp.transpose(outputs, (1, 0, 2))
        loss = jnp.sum((outputs - target) ** 2)
        return (loss, outputs)
    loss, pullback, outputs = jax.vjp(student, map_query, map_key, has_aux=True)
    grad_query_map, grad_key_map = pullback(jnp.ones_like(loss))
    student_out = outputs.astype(jnp.bfloat16).reshape(length, HEADS * DH)
    return (student_out, grad_query_map, grad_key_map)
```

```python
import functools
import math

import jax
import jax.numpy as jnp
from jax import lax
from jax.experimental import pallas as pl
from jax.experimental.pallas import tpu as pltpu
from jax.sharding import PartitionSpec as P

DH = 128


ROPE_BASE = 500000.0
MATMUL_ACCURACY = lax.Precision.DEFAULT


def partner(value, axis, apart):
    mask = 2**apart
    pairs = [(source, source ^ mask) for source in range(lax.axis_size(axis))]
    return lax.ppermute(value, axis, pairs)


def rope_tables(length, width, offset):
    half_width = width // 2
    positions = (offset + jnp.arange(length)).astype(jnp.float32)
    exponent = jnp.arange(half_width).astype(jnp.float32) * (2.0 / width)
    frequency = jnp.power(jnp.float32(ROPE_BASE), -exponent)
    angles = positions[:, None] * frequency[None, :]
    return (jnp.cos(angles), jnp.sin(angles))


def rotate(vectors, cosine, sine):
    half_width = vectors.shape[-1] // 2
    first = vectors[..., :half_width]
    second = vectors[..., half_width:]
    cosine = cosine[:, None, :]
    sine = sine[:, None, :]
    return jnp.concatenate(
        [first * cosine - second * sine, second * cosine + first * sine], axis=-1
    )


def feature_map(vectors, weights):
    logits = jnp.einsum("thd,hdf->thf", vectors, weights, precision=MATMUL_ACCURACY)
    upper = jnp.exp(logits)
    lower = jnp.exp(-logits)
    return jnp.concatenate(
        [upper / jnp.sum(upper, -1, keepdims=True), lower / jnp.sum(lower, -1, keepdims=True)],
        axis=-1,
    )


def teacher_kernel(first_ref, query_ref, key_ref, value_ref, out_ref):
    rows = query_ref.shape[0]
    block = rows // 2 if rows % 2 == 0 else rows
    first = first_ref[0]
    scale = 1.0 / math.sqrt(query_ref.shape[1])
    queries = query_ref[...]

    def scored(start):
        keys = key_ref[pl.ds(start, block), :]
        scores = lax.dot_general(
            queries, keys, (((1,), (1,)), ((), ())), preferred_element_type=jnp.float32
        )
        return scores * scale

    def add(carry, weights, start):
        numerator, denominator = carry
        values = value_ref[pl.ds(start, block), :]
        denominator = denominator + jnp.sum(weights, axis=1, keepdims=True)
        numerator = numerator + jnp.dot(
            weights.astype(jnp.bfloat16), values, preferred_element_type=jnp.float32
        )
        return numerator, denominator

    def earlier(index, carry):
        start = pl.multiple_of(index * block, block)
        return add(carry, jnp.exp(scored(start)), start)

    carry = (
        jnp.zeros((rows, out_ref.shape[1]), jnp.float32),
        jnp.zeros((rows, 1), jnp.float32),
    )
    carry = lax.fori_loop(0, first // block, earlier, carry)
    for part in range(rows // block):
        start = pl.multiple_of(first + part * block, block)
        row = lax.broadcasted_iota(jnp.int32, (rows, block), 0)
        column = lax.broadcasted_iota(jnp.int32, (rows, block), 1) + part * block
        weights = jnp.exp(jnp.where(column <= row, scored(start), -1e30))
        carry = add(carry, weights, start)
    numerator, denominator = carry
    out_ref[...] = (numerator / denominator).astype(out_ref.dtype)


def teacher_attention(first, queries_rot, keys_rot, values):
    rows, width = queries_rot.shape
    span = keys_rot.shape[0]
    return pl.pallas_call(
        teacher_kernel,
        out_shape=jax.ShapeDtypeStruct((rows, width), jnp.bfloat16),
        grid_spec=pltpu.PrefetchScalarGridSpec(
            num_scalar_prefetch=1,
            grid=(width // DH,),
            in_specs=[
                pl.BlockSpec((rows, DH), lambda head, first: (0, head)),
                pl.BlockSpec((span, DH), lambda head, first: (0, 0)),
                pl.BlockSpec((span, DH), lambda head, first: (0, 0)),
            ],
            out_specs=pl.BlockSpec((rows, DH), lambda head, first: (0, head)),
        ),
        compiler_params=pltpu.CompilerParams(vmem_limit_bytes=32 * 1024 * 1024),
        cost_estimate=pl.CostEstimate(
            flops=4 * rows * span * width,
            bytes_accessed=4 * rows * width + 4 * span * DH,
            transcendentals=rows * span * (width // DH),
        ),
    )(jnp.reshape(first, (1,)).astype(jnp.int32), queries_rot, keys_rot, values)


def from_lower(value, shift):
    size = lax.axis_size("seq")
    return lax.ppermute(value, "seq", [(i, i + shift) for i in range(size - shift)])


def from_higher(value, shift):
    size = lax.axis_size("seq")
    return lax.ppermute(value, "seq", [(i + shift, i) for i in range(size - shift)])


def sum_of_others(arrays, receive):
    totals = [jnp.zeros(array.shape, jnp.float32) for array in arrays]
    for shift in range(1, lax.axis_size("seq")):
        for slot, array in enumerate(arrays):
            totals[slot] = totals[slot] + receive(array, shift).astype(jnp.float32)
    return totals


def gather_seq(piece):
    size = lax.axis_size("seq")
    rows = piece.shape[0]
    me = lax.axis_index("seq")
    whole = jnp.zeros((size * rows,) + piece.shape[1:], piece.dtype)
    whole = lax.dynamic_update_slice_in_dim(whole, piece, me * rows, 0)
    for shift in range(1, size):
        source = (me - shift + size) % size
        got = lax.ppermute(piece, "seq", [(i, (i + shift) % size) for i in range(size)])
        whole = lax.dynamic_update_slice_in_dim(whole, got, source * rows, 0)
    return whole


def token_blocks(tokens):
    size = lax.axis_size("head")
    me = lax.axis_index("head")
    if size != 8:
        gathered = lax.all_gather(tokens, "head", axis=1, tiled=True)
        return [(jnp.int32(0), gathered)]
    ring = size // 2
    z, x = me // 2, me % 2

    def up(value):
        return lax.ppermute(value, "head", [(s, (s + 2) % size) for s in range(size)])

    def down(value):
        return lax.ppermute(value, "head", [(s, (s + size - 2) % size) for s in range(size)])

    def across(value):
        return lax.ppermute(value, "head", [(s, s ^ 1) for s in range(size)])

    def index(dz, dx):
        return ((z + dz) % ring) * 2 + (x + dx) % 2

    half = tokens.shape[0] // 2
    below = up(tokens)
    above = down(tokens)
    beside = across(tokens)
    far = jnp.concatenate([up(below[:half]), down(above[half:])], 0)
    beside_below = up(beside)
    beside_above = down(beside)
    beside_far = across(far)
    return [
        (index(0, 0), tokens),
        (index(0, 1), beside),
        (index(ring - 1, 0), below),
        (index(1, 0), above),
        (index(2, 0), far),
        (index(ring - 1, 1), beside_below),
        (index(1, 1), beside_above),
        (index(2, 1), beside_far),
    ]


def per_device_by_rows(tokens, w_query, w_key, w_value, map_query, map_key):
    row_count = tokens.shape[0]
    head_count = w_query.shape[1] // DH
    shared_width = w_key.shape[1]
    w_pair = jnp.concatenate([w_key, w_value], 1)
    query_rows = jnp.zeros((row_count, w_query.shape[1]), jnp.float32)
    pair_rows = jnp.zeros((row_count, w_pair.shape[1]), jnp.float32)
    for position, block in token_blocks(tokens):
        depth = block.shape[1]
        weights = lax.dynamic_slice_in_dim(w_query, position * depth, depth, 0)
        pair_weights = lax.dynamic_slice_in_dim(w_pair, position * depth, depth, 0)
        query_rows = query_rows + jnp.dot(block, weights, preferred_element_type=jnp.float32)
        pair_rows = pair_rows + jnp.dot(block, pair_weights, preferred_element_type=jnp.float32)
    keys = pair_rows[:, :shared_width]
    values = pair_rows[:, shared_width:]
    keys = keys.astype(jnp.bfloat16)
    values = values.astype(jnp.bfloat16)
    if shared_width < DH:
        partner_keys, partner_values = partner((keys, values), "head", 0)
        upper_half = lax.axis_index("head") % 2 == 1
        keys = jnp.where(
            upper_half,
            jnp.concatenate([partner_keys, keys], 1),
            jnp.concatenate([keys, partner_keys], 1),
        )
        values = jnp.where(
            upper_half,
            jnp.concatenate([partner_values, values], 1),
            jnp.concatenate([values, partner_values], 1),
        )
    chain_index = lax.axis_index("seq")
    query_first = chain_index * row_count
    cosine, sine = rope_tables(row_count, DH, query_first)
    queries_rot = rotate(query_rows.reshape(row_count, head_count, DH), cosine, sine).astype(
        jnp.bfloat16
    )
    keys_rot = (
        rotate(keys.astype(jnp.float32).reshape(row_count, 1, DH), cosine, sine)
        .reshape(row_count, DH)
        .astype(jnp.bfloat16)
    )
    pair_all = gather_seq(jnp.concatenate([keys_rot, values], 1))
    teacher = teacher_attention(
        query_first,
        queries_rot.reshape(row_count, head_count * DH),
        pair_all[:, :DH],
        pair_all[:, DH:],
    )
    query_float = queries_rot.astype(jnp.float32)
    key_float = jnp.broadcast_to(
        keys_rot.astype(jnp.float32)[:, None, :], (row_count, head_count, DH)
    )
    value_single_float = values.astype(jnp.float32)
    query_features = feature_map(query_float, map_query)
    key_features = feature_map(key_float, map_key)
    state_local = jnp.einsum(
        "thf,td->hfd", key_features, value_single_float, precision=MATMUL_ACCURACY
    )
    norm_local = jnp.sum(key_features, 0)
    state_before, norm_before = sum_of_others(
        (state_local.astype(jnp.bfloat16), norm_local), from_lower
    )
    local_mask = (jnp.arange(row_count)[None, :] <= jnp.arange(row_count)[:, None]).astype(
        jnp.float32
    )

    def student_local(query_feature_rows, key_feature_rows, state, norm):
        within = (
            jnp.einsum(
                "ueo,aeo->eua", query_feature_rows, key_feature_rows, precision=MATMUL_ACCURACY
            )
            * local_mask[None]
        )
        upper = jnp.einsum("hqk,kd->qhd", within, value_single_float, precision=MATMUL_ACCURACY)
        upper = upper + jnp.einsum(
            "qhf,hfd->qhd", query_feature_rows, state, precision=MATMUL_ACCURACY
        )
        lower = jnp.transpose(jnp.sum(within, -1)) + jnp.einsum(
            "qhf,hf->qh", query_feature_rows, norm, precision=MATMUL_ACCURACY
        )
        return upper / lower[..., None]

    student, pullback = jax.vjp(
        student_local, query_features, key_features, state_before, norm_before
    )
    student_out = student.astype(jnp.bfloat16).reshape(row_count, head_count * DH)
    target = teacher.reshape(row_count, head_count, DH).astype(jnp.float32)
    grad_student = 2.0 * (student - target)
    grad_query_feat, grad_key_feat, grad_state, grad_norm = pullback(grad_student)
    state_after, norm_after = sum_of_others(
        (grad_state.astype(jnp.bfloat16), grad_norm), from_higher
    )
    grad_key_feat = (
        grad_key_feat
        + jnp.einsum("td,hfd->thf", value_single_float, state_after, precision=MATMUL_ACCURACY)
        + norm_after[None]
    )
    unused_query, query_backward = jax.vjp(
        lambda weights: feature_map(query_float, weights), map_query
    )
    unused_key, pull_key = jax.vjp(lambda weights: feature_map(key_float, weights), map_key)
    grad_query = query_backward(grad_query_feat)[0]
    grad_key = pull_key(grad_key_feat)[0]
    features = grad_query.shape[-1]
    grads = jnp.concatenate([grad_query, grad_key], -1)
    size = lax.axis_size("seq")
    if size & (size - 1):
        grads = lax.psum(grads, "seq")
    else:
        apart = 0
        while 2**apart < size:
            if apart > 0:
                sent = grads.astype(jnp.bfloat16)
                grads = sent.astype(jnp.float32) + partner(sent, "seq", apart).astype(jnp.float32)
            else:
                grads = grads + partner(grads, "seq", apart)
            apart += 1
    grad_query, grad_key = grads[..., :features], grads[..., features:]
    return (student_out, grad_query, grad_key)


F32 = jnp.float32
BF16 = jnp.bfloat16

def dot_nn(a, b):
    return lax.dot_general(a, b, (((1,), (0,)), ((), ())), preferred_element_type=F32)
def dot_nt(a, b):
    return lax.dot_general(a, b, (((1,), (1,)), ((), ())), preferred_element_type=F32)
def dot_tn(a, b):
    return lax.dot_general(a, b, (((0,), (0,)), ((), ())), preferred_element_type=F32)

def split(v):
    high = v.astype(BF16)
    low = (v - high.astype(F32)).astype(BF16)
    return high, low

def half_sums(v, ones):
    high, low = split(v)
    return dot_nn(jnp.concatenate([high, low], 1), ones)

def attention_kernel(C, W, q_ref, kv_ref, mq_ref, mk_ref, out_ref, grad_ref,
                     vaug, tch, qf, kf, qfb, kfb, dk, gu, state, gsum, mq, mk, wq, wk):
    T = q_ref.shape[0]
    H = q_ref.shape[1] // DH
    tiles = T // C
    scale = math.log2(math.e) / math.sqrt(DH)
    r = lax.broadcasted_iota(jnp.int32, (2 * DH, DH), 0)
    c = lax.broadcasted_iota(jnp.int32, (2 * DH, DH), 1)
    half = DH // 2
    ones = jnp.where((r % DH) // half == c // half, 1.0, 0.0).astype(BF16)
    row = lax.broadcasted_iota(jnp.int32, (C, C), 0)
    column = lax.broadcasted_iota(jnp.int32, (C, C), 1)
    causal = column <= row
    for h in range(H):
        for src, dst in ((mq_ref, wq), (mk_ref, wk)):
            w = src[h]
            high, low = split(jnp.concatenate([w, -w], 1))
            dst[h] = jnp.concatenate([high, low], 0)
    state[...] = jnp.zeros_like(state)
    gsum[...] = jnp.zeros_like(gsum)
    mq[...] = jnp.zeros_like(mq)
    mk[...] = jnp.zeros_like(mk)

    def rows_of(i):
        return pl.ds(pl.multiple_of(i * C, C), C)

    def features(i, carry):
        rows = rows_of(i)
        k = kv_ref[rows, :DH]
        vaug[rows, :DH] = kv_ref[rows, DH:]
        vaug[rows, DH:] = jnp.ones((C, DH), BF16)
        k2 = jnp.concatenate([k, k], 1)
        for h in range(H):
            cols = slice(h * DH, (h + 1) * DH)
            q = q_ref[rows, cols]
            for x2, w, f, fb in ((jnp.concatenate([q, q], 1), wq, qf, qfb), (k2, wk, kf, kfb)):
                e = jnp.exp(dot_nn(x2, w[h]))
                phi = e / half_sums(e, ones)
                f[rows, cols] = phi
                fb[rows, cols] = phi.astype(BF16)
        return carry
    lax.fori_loop(0, tiles, features, 0)

    def phi_back(phi, d):
        return (phi * (d - half_sums(d * phi, ones))).astype(BF16)

    big = W // C
    heads = range(H)

    def teach(n, carry):
        first = n * big
        rows = pl.ds(pl.multiple_of(n * W, W), W)
        q = jnp.concatenate([q_ref[rows, h * DH:(h + 1) * DH] for h in heads], 0)

        def earlier(j, acc):
            seen = pl.ds(pl.multiple_of(j * W, W), W)
            s = dot_nt(q, kv_ref[seen, :DH]) * scale
            return acc + dot_nn(jnp.exp2(s).astype(BF16), vaug[seen, :])
        acc = lax.fori_loop(0, n, earlier, jnp.zeros((H * W, 2 * DH), F32))
        parts = []
        for b in range(big):
            seen = pl.ds(pl.multiple_of(n * W + b * C, C), C)
            q = jnp.concatenate([q_ref[pl.ds(pl.multiple_of(n * W + b * C, C), W - b * C), h * DH:(h + 1) * DH] for h in heads], 0)
            s = dot_nt(q, kv_ref[seen, :DH]) * scale
            left = W - b * C
            s = jnp.concatenate([x for h in heads for x in
                                 [jnp.where(causal, s[h * left:h * left + C], -1e30), s[h * left + C:(h + 1) * left]]], 0) if left > C else jnp.concatenate([jnp.where(causal, s[h * C:(h + 1) * C], -1e30) for h in heads], 0)
            p = dot_nn(jnp.exp2(s).astype(BF16), vaug[seen, :])
            parts.append(p)
        for h in heads:
            for b in range(big):
                v = acc[h * W + b * C:h * W + (b + 1) * C]
                for b2 in range(b + 1):
                    left = W - b2 * C
                    lo = h * left + (b - b2) * C
                    v = v + parts[b2][lo:lo + C]
                tch[pl.ds(pl.multiple_of(n * W + b * C, C), C), h * DH:(h + 1) * DH] = (v[:, :DH] / v[:, DH:]).astype(BF16)
        return carry
    lax.fori_loop(0, T // W, teach, 0)

    def forward(i, carry):
        rows = rows_of(i)
        va = vaug[rows, :]
        cols = [slice(h * DH, (h + 1) * DH) for h in heads]
        fq = [qfb[rows, cols[h]] for h in heads]
        fk = [kfb[rows, cols[h]] for h in heads]
        st = [state[h] for h in heads]
        stb = [x.astype(BF16) for x in st]
        a = [jnp.where(causal, dot_nt(fq[h], fk[h]), 0.0).astype(BF16) for h in heads]
        av = dot_nn(jnp.concatenate(a, 0), va)
        dua = []
        for h in heads:
            nd = av[h * C:(h + 1) * C] + dot_nn(fq[h], stb[h])
            inv = 1.0 / nd[:, DH:]
            y = nd[:, :DH] * inv
            out_ref[rows, cols[h]] = y.astype(out_ref.dtype)
            du = ((2.0 * (y - tch[rows, cols[h]].astype(F32))) * inv).astype(BF16)
            dl = jnp.sum(du.astype(F32) * y, 1, keepdims=True) * (-1.0 / half)
            dl_high, dl_low = split(dl)
            dua.append(jnp.concatenate([du, jnp.broadcast_to(dl_high, (C, half)), jnp.broadcast_to(dl_low, (C, half))], 1))
            state[h] = st[h] + dot_tn(fk[h], va)
        dall = dot_nt(jnp.concatenate(dua, 0), va)
        for h in heads:
            da = jnp.where(causal, dall[h * C:(h + 1) * C], 0.0).astype(BF16)
            dq = dot_nn(da, fk[h]) + dot_nt(dua[h], stb[h])
            dk[rows, cols[h]] = dot_tn(da, fq[h])
            gu[i, h] = dot_tn(fq[h], dua[h])
            g = phi_back(qf[rows, cols[h]], dq)
            mq[h] += dot_tn(q_ref[rows, cols[h]], g)
        return carry
    lax.fori_loop(0, tiles, forward, 0)

    def backward(n, carry):
        i = tiles - 1 - n
        rows = rows_of(i)
        va = vaug[rows, :]
        keys = kv_ref[rows, :DH]
        for h in range(H):
            cols = slice(h * DH, (h + 1) * DH)
            d = dk[rows, cols] + dot_nt(va, gsum[h].astype(BF16))
            g = phi_back(kf[rows, cols], d)
            mk[h] += dot_tn(keys, g)
            gsum[h] += gu[i, h]
        return carry
    lax.fori_loop(0, tiles, backward, 0)
    for h in range(H):
        a, b = mq[h], mk[h]
        grad_ref[h] = jnp.concatenate([a[:, :half] - a[:, half:], b[:, :half] - b[:, half:]], 1)

def attention(q, kv, map_query, map_key, W, C=256):
    T, width = q.shape
    H = width // DH
    V = lambda *s: pltpu.VMEM(s, F32)
    B = lambda *s: pltpu.VMEM(s, BF16)
    vm = pl.BlockSpec(memory_space=pltpu.VMEM)
    return pl.pallas_call(
        functools.partial(attention_kernel, C, W),
        out_shape=(jax.ShapeDtypeStruct((T, width), BF16), jax.ShapeDtypeStruct((H, DH, DH), F32)),
        in_specs=[vm] * 4, out_specs=(vm, vm),
        scratch_shapes=[B(T, 2 * DH), B(T, width), V(T, width), V(T, width), B(T, width), B(T, width), V(T, width),
                        V(T // C, H, DH, 2 * DH), V(H, DH, 2 * DH), V(H, DH, 2 * DH), V(H, DH, DH), V(H, DH, DH),
                        B(H, 2 * DH, DH), B(H, 2 * DH, DH)],
        compiler_params=pltpu.CompilerParams(vmem_limit_bytes=60 * 2**20),
        cost_estimate=pl.CostEstimate(flops=4 * T * T * width, bytes_accessed=8 * T * width, transcendentals=T * T * H),
    )(q, kv, map_query, map_key)


def project(tokens, w_query, w_key, w_value):
    w_pair = jnp.concatenate([w_key, w_value], 1)
    query_rows = jnp.zeros((tokens.shape[0], w_query.shape[1]), F32)
    pair_rows = jnp.zeros((tokens.shape[0], w_pair.shape[1]), F32)
    for position, block in token_blocks(tokens):
        depth = block.shape[1]
        weights = lax.dynamic_slice_in_dim(w_query, position * depth, depth, 0)
        pair_weights = lax.dynamic_slice_in_dim(w_pair, position * depth, depth, 0)
        query_rows = query_rows + jnp.dot(block, weights, preferred_element_type=F32)
        pair_rows = pair_rows + jnp.dot(block, pair_weights, preferred_element_type=F32)
    return query_rows, pair_rows.astype(BF16)


def per_device_by_heads(tokens, w_query, w_key, w_value, map_query, map_key):
    row_count = tokens.shape[0]
    head_count = w_query.shape[1] // DH
    size = lax.axis_size("seq")
    me = lax.axis_index("seq")
    mine = head_count // size
    query_rows, pair = project(tokens, w_query, w_key, w_value)
    cosine, sine = rope_tables(row_count, DH, me * row_count)
    queries = rotate(query_rows.reshape(row_count, head_count, DH), cosine, sine).astype(BF16)
    keys = rotate(pair[:, :DH].astype(F32).reshape(row_count, 1, DH), cosine, sine)
    keys = keys.reshape(row_count, DH).astype(BF16)
    pair_all = gather_seq(jnp.concatenate([keys, pair[:, DH:]], 1))
    queries = lax.all_to_all(
        queries.reshape(row_count, head_count * DH), "seq", 1, 0, tiled=True
    )
    query_maps = lax.dynamic_slice_in_dim(map_query, me * mine, mine, 0)
    key_maps = lax.dynamic_slice_in_dim(map_key, me * mine, mine, 0)
    out, grads = attention(queries, pair_all, query_maps, key_maps, row_count)
    student_out = lax.all_to_all(out, "seq", 0, 1, tiled=True)
    grads = gather_seq(grads)
    features = map_query.shape[-1]
    return student_out, grads[..., :features], grads[..., features:]


def fits(mesh, w_query, w_key):
    heads = w_query.shape[1] // mesh.shape["head"]
    return w_key.shape[1] // mesh.shape["head"] == DH and (heads // DH) % mesh.shape["seq"] == 0


def solution(mesh):
    in_specs = (
        P("seq", "head"),
        P(None, "head"),
        P(None, "head"),
        P(None, "head"),
        P("head", None, None),
        P("head", None, None),
    )
    out_specs = (P("seq", "head"), P("head", None, None), P("head", None, None))

    def run(tokens, w_query, w_key, w_value, map_query, map_key):
        body = per_device_by_heads if fits(mesh, w_query, w_key) else per_device_by_rows
        return jax.shard_map(
            body, mesh=mesh, in_specs=in_specs, out_specs=out_specs, check_vma=False
        )(tokens, w_query, w_key, w_value, map_query, map_key)

    return run
```

```python
import functools
import math

import jax
import jax.numpy as jnp
from jax import lax
from jax.experimental import pallas as pl
from jax.experimental.pallas import tpu as pltpu
from jax.sharding import PartitionSpec as P

DH = 128


ROPE_BASE = 500000.0
MATMUL_ACCURACY = lax.Precision.DEFAULT


def partner(value, axis, apart):
    mask = 2**apart
    pairs = [(source, source ^ mask) for source in range(lax.axis_size(axis))]
    return lax.ppermute(value, axis, pairs)


def rope_tables(length, width, offset):
    half_width = width // 2
    positions = (offset + jnp.arange(length)).astype(jnp.float32)
    exponent = jnp.arange(half_width).astype(jnp.float32) * (2.0 / width)
    frequency = jnp.power(jnp.float32(ROPE_BASE), -exponent)
    angles = positions[:, None] * frequency[None, :]
    return (jnp.cos(angles), jnp.sin(angles))


def rotate(vectors, cosine, sine):
    half_width = vectors.shape[-1] // 2
    first = vectors[..., :half_width]
    second = vectors[..., half_width:]
    cosine = cosine[:, None, :]
    sine = sine[:, None, :]
    return jnp.concatenate(
        [first * cosine - second * sine, second * cosine + first * sine], axis=-1
    )


def feature_map(vectors, weights):
    logits = jnp.einsum("thd,hdf->thf", vectors, weights, precision=MATMUL_ACCURACY)
    upper = jnp.exp(logits)
    lower = jnp.exp(-logits)
    return jnp.concatenate(
        [upper / jnp.sum(upper, -1, keepdims=True), lower / jnp.sum(lower, -1, keepdims=True)],
        axis=-1,
    )


def teacher_kernel(first_ref, query_ref, key_ref, value_ref, out_ref):
    rows = query_ref.shape[0]
    block = rows // 2 if rows % 2 == 0 else rows
    first = first_ref[0]
    scale = 1.0 / math.sqrt(query_ref.shape[1])
    queries = query_ref[...]

    def scored(start):
        keys = key_ref[pl.ds(start, block), :]
        scores = lax.dot_general(
            queries, keys, (((1,), (1,)), ((), ())), preferred_element_type=jnp.float32
        )
        return scores * scale

    def add(carry, weights, start):
        numerator, denominator = carry
        values = value_ref[pl.ds(start, block), :]
        denominator = denominator + jnp.sum(weights, axis=1, keepdims=True)
        numerator = numerator + jnp.dot(
            weights.astype(jnp.bfloat16), values, preferred_element_type=jnp.float32
        )
        return numerator, denominator

    def earlier(index, carry):
        start = pl.multiple_of(index * block, block)
        return add(carry, jnp.exp(scored(start)), start)

    carry = (
        jnp.zeros((rows, out_ref.shape[1]), jnp.float32),
        jnp.zeros((rows, 1), jnp.float32),
    )
    carry = lax.fori_loop(0, first // block, earlier, carry)
    for part in range(rows // block):
        start = pl.multiple_of(first + part * block, block)
        row = lax.broadcasted_iota(jnp.int32, (rows, block), 0)
        column = lax.broadcasted_iota(jnp.int32, (rows, block), 1) + part * block
        weights = jnp.exp(jnp.where(column <= row, scored(start), -1e30))
        carry = add(carry, weights, start)
    numerator, denominator = carry
    out_ref[...] = (numerator / denominator).astype(out_ref.dtype)


def teacher_attention(first, queries_rot, keys_rot, values):
    rows, width = queries_rot.shape
    span = keys_rot.shape[0]
    return pl.pallas_call(
        teacher_kernel,
        out_shape=jax.ShapeDtypeStruct((rows, width), jnp.bfloat16),
        grid_spec=pltpu.PrefetchScalarGridSpec(
            num_scalar_prefetch=1,
            grid=(width // DH,),
            in_specs=[
                pl.BlockSpec((rows, DH), lambda head, first: (0, head)),
                pl.BlockSpec((span, DH), lambda head, first: (0, 0)),
                pl.BlockSpec((span, DH), lambda head, first: (0, 0)),
            ],
            out_specs=pl.BlockSpec((rows, DH), lambda head, first: (0, head)),
        ),
        compiler_params=pltpu.CompilerParams(vmem_limit_bytes=32 * 1024 * 1024),
        cost_estimate=pl.CostEstimate(
            flops=4 * rows * span * width,
            bytes_accessed=4 * rows * width + 4 * span * DH,
            transcendentals=rows * span * (width // DH),
        ),
    )(jnp.reshape(first, (1,)).astype(jnp.int32), queries_rot, keys_rot, values)


def from_lower(value, shift):
    size = lax.axis_size("seq")
    return lax.ppermute(value, "seq", [(i, i + shift) for i in range(size - shift)])


def from_higher(value, shift):
    size = lax.axis_size("seq")
    return lax.ppermute(value, "seq", [(i + shift, i) for i in range(size - shift)])


def sum_of_others(arrays, receive):
    totals = [jnp.zeros(array.shape, jnp.float32) for array in arrays]
    for shift in range(1, lax.axis_size("seq")):
        for slot, array in enumerate(arrays):
            totals[slot] = totals[slot] + receive(array, shift).astype(jnp.float32)
    return totals


def gather_seq(piece):
    size = lax.axis_size("seq")
    rows = piece.shape[0]
    me = lax.axis_index("seq")
    whole = jnp.zeros((size * rows,) + piece.shape[1:], piece.dtype)
    whole = lax.dynamic_update_slice_in_dim(whole, piece, me * rows, 0)
    for shift in range(1, size):
        source = (me - shift + size) % size
        got = lax.ppermute(piece, "seq", [(i, (i + shift) % size) for i in range(size)])
        whole = lax.dynamic_update_slice_in_dim(whole, got, source * rows, 0)
    return whole


def token_blocks(tokens):
    size = lax.axis_size("head")
    me = lax.axis_index("head")
    if size != 8:
        gathered = lax.all_gather(tokens, "head", axis=1, tiled=True)
        return [(jnp.int32(0), gathered)]
    ring = size // 2
    z, x = me // 2, me % 2

    def up(value):
        return lax.ppermute(value, "head", [(s, (s + 2) % size) for s in range(size)])

    def down(value):
        return lax.ppermute(value, "head", [(s, (s + size - 2) % size) for s in range(size)])

    def across(value):
        return lax.ppermute(value, "head", [(s, s ^ 1) for s in range(size)])

    def index(dz, dx):
        return ((z + dz) % ring) * 2 + (x + dx) % 2

    half = tokens.shape[0] // 2
    below = up(tokens)
    above = down(tokens)
    beside = across(tokens)
    far = jnp.concatenate([up(below[:half]), down(above[half:])], 0)
    beside_below = up(beside)
    beside_above = down(beside)
    beside_far = across(far)
    return [
        (index(0, 0), tokens),
        (index(0, 1), beside),
        (index(ring - 1, 0), below),
        (index(1, 0), above),
        (index(2, 0), far),
        (index(ring - 1, 1), beside_below),
        (index(1, 1), beside_above),
        (index(2, 1), beside_far),
    ]


def per_device_by_rows(tokens, w_query, w_key, w_value, map_query, map_key):
    row_count = tokens.shape[0]
    head_count = w_query.shape[1] // DH
    shared_width = w_key.shape[1]
    w_pair = jnp.concatenate([w_key, w_value], 1)
    query_rows = jnp.zeros((row_count, w_query.shape[1]), jnp.float32)
    pair_rows = jnp.zeros((row_count, w_pair.shape[1]), jnp.float32)
    for position, block in token_blocks(tokens):
        depth = block.shape[1]
        weights = lax.dynamic_slice_in_dim(w_query, position * depth, depth, 0)
        pair_weights = lax.dynamic_slice_in_dim(w_pair, position * depth, depth, 0)
        query_rows = query_rows + jnp.dot(block, weights, preferred_element_type=jnp.float32)
        pair_rows = pair_rows + jnp.dot(block, pair_weights, preferred_element_type=jnp.float32)
    keys = pair_rows[:, :shared_width]
    values = pair_rows[:, shared_width:]
    keys = keys.astype(jnp.bfloat16)
    values = values.astype(jnp.bfloat16)
    if shared_width < DH:
        partner_keys, partner_values = partner((keys, values), "head", 0)
        upper_half = lax.axis_index("head") % 2 == 1
        keys = jnp.where(
            upper_half,
            jnp.concatenate([partner_keys, keys], 1),
            jnp.concatenate([keys, partner_keys], 1),
        )
        values = jnp.where(
            upper_half,
            jnp.concatenate([partner_values, values], 1),
            jnp.concatenate([values, partner_values], 1),
        )
    chain_index = lax.axis_index("seq")
    query_first = chain_index * row_count
    cosine, sine = rope_tables(row_count, DH, query_first)
    queries_rot = rotate(query_rows.reshape(row_count, head_count, DH), cosine, sine).astype(
        jnp.bfloat16
    )
    keys_rot = (
        rotate(keys.astype(jnp.float32).reshape(row_count, 1, DH), cosine, sine)
        .reshape(row_count, DH)
        .astype(jnp.bfloat16)
    )
    pair_all = gather_seq(jnp.concatenate([keys_rot, values], 1))
    teacher = teacher_attention(
        query_first,
        queries_rot.reshape(row_count, head_count * DH),
        pair_all[:, :DH],
        pair_all[:, DH:],
    )
    query_float = queries_rot.astype(jnp.float32)
    key_float = jnp.broadcast_to(
        keys_rot.astype(jnp.float32)[:, None, :], (row_count, head_count, DH)
    )
    value_single_float = values.astype(jnp.float32)
    query_features = feature_map(query_float, map_query)
    key_features = feature_map(key_float, map_key)
    state_local = jnp.einsum(
        "thf,td->hfd", key_features, value_single_float, precision=MATMUL_ACCURACY
    )
    norm_local = jnp.sum(key_features, 0)
    state_before, norm_before = sum_of_others(
        (state_local.astype(jnp.bfloat16), norm_local), from_lower
    )
    local_mask = (jnp.arange(row_count)[None, :] <= jnp.arange(row_count)[:, None]).astype(
        jnp.float32
    )

    def student_local(query_feature_rows, key_feature_rows, state, norm):
        within = (
            jnp.einsum(
                "ueo,aeo->eua", query_feature_rows, key_feature_rows, precision=MATMUL_ACCURACY
            )
            * local_mask[None]
        )
        upper = jnp.einsum("hqk,kd->qhd", within, value_single_float, precision=MATMUL_ACCURACY)
        upper = upper + jnp.einsum(
            "qhf,hfd->qhd", query_feature_rows, state, precision=MATMUL_ACCURACY
        )
        lower = jnp.transpose(jnp.sum(within, -1)) + jnp.einsum(
            "qhf,hf->qh", query_feature_rows, norm, precision=MATMUL_ACCURACY
        )
        return upper / lower[..., None]

    student, pullback = jax.vjp(
        student_local, query_features, key_features, state_before, norm_before
    )
    student_out = student.astype(jnp.bfloat16).reshape(row_count, head_count * DH)
    target = teacher.reshape(row_count, head_count, DH).astype(jnp.float32)
    grad_student = 2.0 * (student - target)
    grad_query_feat, grad_key_feat, grad_state, grad_norm = pullback(grad_student)
    state_after, norm_after = sum_of_others(
        (grad_state.astype(jnp.bfloat16), grad_norm), from_higher
    )
    grad_key_feat = (
        grad_key_feat
        + jnp.einsum("td,hfd->thf", value_single_float, state_after, precision=MATMUL_ACCURACY)
        + norm_after[None]
    )
    unused_query, query_backward = jax.vjp(
        lambda weights: feature_map(query_float, weights), map_query
    )
    unused_key, pull_key = jax.vjp(lambda weights: feature_map(key_float, weights), map_key)
    grad_query = query_backward(grad_query_feat)[0]
    grad_key = pull_key(grad_key_feat)[0]
    features = grad_query.shape[-1]
    grads = jnp.concatenate([grad_query, grad_key], -1)
    size = lax.axis_size("seq")
    if size & (size - 1):
        grads = lax.psum(grads, "seq")
    else:
        apart = 0
        while 2**apart < size:
            if apart > 0:
                sent = grads.astype(jnp.bfloat16)
                grads = sent.astype(jnp.float32) + partner(sent, "seq", apart).astype(jnp.float32)
            else:
                grads = grads + partner(grads, "seq", apart)
            apart += 1
    grad_query, grad_key = grads[..., :features], grads[..., features:]
    return (student_out, grad_query, grad_key)


F32 = jnp.float32
BF16 = jnp.bfloat16
MESH = pl.DeviceIdType.MESH


def dot_nn(a, b):
    return lax.dot_general(a, b, (((1,), (0,)), ((), ())), preferred_element_type=F32)
def dot_nt(a, b):
    return lax.dot_general(a, b, (((1,), (1,)), ((), ())), preferred_element_type=F32)
def dot_tn(a, b):
    return lax.dot_general(a, b, (((0,), (0,)), ((), ())), preferred_element_type=F32)

def split(v):
    high = v.astype(BF16)
    low = (v - high.astype(F32)).astype(BF16)
    return high, low

def half_sums(v, ones):
    high, low = split(v)
    return dot_nn(jnp.concatenate([high, low], 1), ones)

def attention_kernel(C, q_hbm, kv_hbm, mapq_hbm, mapk_hbm, out_hbm, gradq_ref, gradk_ref,
                     q_ref, kv_ref, mq_ref, mk_ref, out_ref, vaug, tch, qf, kf, qfb, kfb, dk, gu, state, gsum, mq, mk,
                     wq, wk, land, load_sem, out_send, out_recv, own_sem, grad_send, grad_recv):
    T = q_ref.shape[0]
    W = out_hbm.shape[0]
    size = lax.axis_size("seq")
    me = lax.axis_index("seq")
    barrier = pltpu.get_barrier_semaphore()
    for shift in range(1, size):
        pl.semaphore_signal(barrier, 1, device_id={"seq": lax.rem(me + shift, size)}, device_id_type=MESH)
    heads_here = pl.ds(me * (q_ref.shape[1] // DH), q_ref.shape[1] // DH)
    loads = [pltpu.make_async_copy(src, dst, load_sem.at[n]) for n, (src, dst) in enumerate((
        (mapq_hbm.at[heads_here], mq_ref), (mapk_hbm.at[heads_here], mk_ref), (kv_hbm, kv_ref), (q_hbm, q_ref)))]
    for copy in loads:
        copy.start()
    pl.semaphore_wait(barrier, size - 1)
    for copy in loads:
        copy.wait()
    H = q_ref.shape[1] // DH
    tiles = T // C
    scale = math.log2(math.e) / math.sqrt(DH)
    r = lax.broadcasted_iota(jnp.int32, (2 * DH, DH), 0)
    c = lax.broadcasted_iota(jnp.int32, (2 * DH, DH), 1)
    half = DH // 2
    ones = jnp.where((r % DH) // half == c // half, 1.0, 0.0).astype(BF16)
    row = lax.broadcasted_iota(jnp.int32, (C, C), 0)
    column = lax.broadcasted_iota(jnp.int32, (C, C), 1)
    causal = column <= row
    for h in range(H):
        for src, dst in ((mq_ref, wq), (mk_ref, wk)):
            w = src[h]
            high, low = split(jnp.concatenate([w, -w], 1))
            dst[h] = jnp.concatenate([high, low], 0)
    state[...] = jnp.zeros_like(state)
    gsum[...] = jnp.zeros_like(gsum)
    mq[...] = jnp.zeros_like(mq)
    mk[...] = jnp.zeros_like(mk)

    def rows_of(i):
        return pl.ds(pl.multiple_of(i * C, C), C)

    def features(i, carry):
        rows = rows_of(i)
        k = kv_ref[rows, :DH]
        vaug[rows, :DH] = kv_ref[rows, DH:]
        vaug[rows, DH:] = jnp.ones((C, DH), BF16)
        k2 = jnp.concatenate([k, k], 1)
        for h in range(H):
            cols = slice(h * DH, (h + 1) * DH)
            q = q_ref[rows, cols]
            for x2, w, f, fb in ((jnp.concatenate([q, q], 1), wq, qf, qfb), (k2, wk, kf, kfb)):
                e = jnp.exp(dot_nn(x2, w[h]))
                phi = e / half_sums(e, ones)
                f[rows, cols] = phi
                fb[rows, cols] = phi.astype(BF16)
        return carry
    lax.fori_loop(0, tiles, features, 0)

    def phi_back(phi, d):
        return (phi * (d - half_sums(d * phi, ones))).astype(BF16)

    big = W // C
    heads = range(H)
    width = H * DH

    def out_copy(i, local):
        owner = i // big
        to = out_hbm.at[pl.ds(pl.multiple_of(lax.rem(i, big) * C, C), C), pl.ds(pl.multiple_of(me * width, width), width)]
        if local:
            return pltpu.make_async_copy(out_ref.at[rows_of(i)], to, own_sem.at[lax.rem(i, big)])
        return pltpu.make_async_remote_copy(
            src_ref=out_ref.at[rows_of(i)], dst_ref=to, send_sem=out_send.at[i], recv_sem=out_recv.at[lax.rem(i, big), me],
            device_id={"seq": owner}, device_id_type=MESH)

    def give(i, act_local, act_remote):
        @pl.when(i // big == me)
        def _():
            act_local(out_copy(i, True))
        @pl.when(i // big != me)
        def _():
            act_remote(out_copy(i, False))

    start = lambda copy: copy.start()

    def grad_copy(kind, shift):
        return pltpu.make_async_remote_copy(
            src_ref=land.at[kind, me], dst_ref=land.at[kind, me], send_sem=grad_send.at[kind, shift],
            recv_sem=grad_recv.at[kind, shift], device_id={"seq": lax.rem(me + shift, size)}, device_id_type=MESH)

    def give_grads(kind, total):
        for h in heads:
            v = total[h]
            land[kind, me, :, h * half:(h + 1) * half] = v[:, :half] - v[:, half:]
        for shift in range(1, size):
            grad_copy(kind, shift).start()

    def teach(n, carry):
        first = n * big
        rows = pl.ds(pl.multiple_of(n * W, W), W)
        q = jnp.concatenate([q_ref[rows, h * DH:(h + 1) * DH] for h in heads], 0)

        def earlier(j, acc):
            seen = pl.ds(pl.multiple_of(j * W, W), W)
            s = dot_nt(q, kv_ref[seen, :DH]) * scale
            return acc + dot_nn(jnp.exp2(s).astype(BF16), vaug[seen, :])
        acc = lax.fori_loop(0, n, earlier, jnp.zeros((H * W, 2 * DH), F32))
        parts = []
        for b in range(big):
            seen = pl.ds(pl.multiple_of(n * W + b * C, C), C)
            q = jnp.concatenate([q_ref[pl.ds(pl.multiple_of(n * W + b * C, C), W - b * C), h * DH:(h + 1) * DH] for h in heads], 0)
            s = dot_nt(q, kv_ref[seen, :DH]) * scale
            left = W - b * C
            s = jnp.concatenate([x for h in heads for x in
                                 [jnp.where(causal, s[h * left:h * left + C], -1e30), s[h * left + C:(h + 1) * left]]], 0) if left > C else jnp.concatenate([jnp.where(causal, s[h * C:(h + 1) * C], -1e30) for h in heads], 0)
            p = dot_nn(jnp.exp2(s).astype(BF16), vaug[seen, :])
            parts.append(p)
        for h in heads:
            for b in range(big):
                v = acc[h * W + b * C:h * W + (b + 1) * C]
                for b2 in range(b + 1):
                    left = W - b2 * C
                    lo = h * left + (b - b2) * C
                    v = v + parts[b2][lo:lo + C]
                tch[pl.ds(pl.multiple_of(n * W + b * C, C), C), h * DH:(h + 1) * DH] = (v[:, :DH] / v[:, DH:]).astype(BF16)
        return carry
    lax.fori_loop(0, T // W, teach, 0)

    def forward(i, carry):
        @pl.when(i > 0)
        def _():
            give(i - 1, start, start)
        rows = rows_of(i)
        va = vaug[rows, :]
        cols = [slice(h * DH, (h + 1) * DH) for h in heads]
        fq = [qfb[rows, cols[h]] for h in heads]
        fk = [kfb[rows, cols[h]] for h in heads]
        st = [state[h] for h in heads]
        stb = [x.astype(BF16) for x in st]
        a = [jnp.where(causal, dot_nt(fq[h], fk[h]), 0.0).astype(BF16) for h in heads]
        av = dot_nn(jnp.concatenate(a, 0), va)
        dua = []
        for h in heads:
            nd = av[h * C:(h + 1) * C] + dot_nn(fq[h], stb[h])
            inv = 1.0 / nd[:, DH:]
            y = nd[:, :DH] * inv
            out_ref[rows, cols[h]] = y.astype(out_ref.dtype)
            du = ((2.0 * (y - tch[rows, cols[h]].astype(F32))) * inv).astype(BF16)
            dl = jnp.sum(du.astype(F32) * y, 1, keepdims=True) * (-1.0 / half)
            dl_high, dl_low = split(dl)
            dua.append(jnp.concatenate([du, jnp.broadcast_to(dl_high, (C, half)), jnp.broadcast_to(dl_low, (C, half))], 1))
            state[h] = st[h] + dot_tn(fk[h], va)
        dall = dot_nt(jnp.concatenate(dua, 0), va)
        for h in heads:
            da = jnp.where(causal, dall[h * C:(h + 1) * C], 0.0).astype(BF16)
            dq = dot_nn(da, fk[h]) + dot_nt(dua[h], stb[h])
            dk[rows, cols[h]] = dot_tn(da, fq[h])
            gu[i, h] = dot_tn(fq[h], dua[h])
            g = phi_back(qf[rows, cols[h]], dq)
            mq[h] += dot_tn(q_ref[rows, cols[h]], g)
        return carry
    lax.fori_loop(0, tiles, forward, 0)
    give(tiles - 1, start, start)
    give_grads(0, mq)

    def backward(n, carry):
        i = tiles - 1 - n
        rows = rows_of(i)
        va = vaug[rows, :]
        keys = kv_ref[rows, :DH]
        for h in range(H):
            cols = slice(h * DH, (h + 1) * DH)
            d = dk[rows, cols] + dot_nt(va, gsum[h].astype(BF16))
            g = phi_back(kf[rows, cols], d)
            mk[h] += dot_tn(keys, g)
            gsum[h] += gu[i, h]
        return carry
    lax.fori_loop(0, tiles, backward, 0)
    give_grads(1, mk)

    def finish(i, carry):
        give(i, lambda copy: copy.wait(), lambda copy: copy.wait_send())
        return carry
    lax.fori_loop(0, tiles, finish, 0)
    for b in range(big):
        for shift in range(1, size):
            source = lax.rem(me + shift, size)
            pltpu.make_async_remote_copy(
                src_ref=out_ref.at[rows_of(b)],
                dst_ref=out_hbm.at[pl.ds(b * C, C), pl.ds(pl.multiple_of(source * width, width), width)],
                send_sem=out_send.at[b], recv_sem=out_recv.at[b, source],
                device_id={"seq": source}, device_id_type=MESH).wait_recv()
    for kind, ref in ((0, gradq_ref), (1, gradk_ref)):
        for shift in range(1, size):
            grad_copy(kind, shift).wait()
        for n in range(size):
            for h in heads:
                ref[n * H + h] = land[kind, n, :, h * half:(h + 1) * half]


def attention(q, kv, map_query, map_key, rows, C=256):
    T, width = q.shape
    H = width // DH
    count = map_query.shape[0]
    size = lax.axis_size("seq")
    V = lambda *s: pltpu.VMEM(s, F32)
    B = lambda *s: pltpu.VMEM(s, BF16)
    dma = pltpu.SemaphoreType.DMA
    vm = pl.BlockSpec(memory_space=pltpu.VMEM)
    anywhere = pl.BlockSpec(memory_space=pl.ANY)
    grads = jax.ShapeDtypeStruct(map_query.shape, F32)
    maps = (H,) + map_query.shape[1:]
    tiles = T // C
    return pl.pallas_call(
        functools.partial(attention_kernel, C),
        out_shape=(jax.ShapeDtypeStruct((rows, count * DH), BF16), grads, grads),
        in_specs=[anywhere] * 4,
        out_specs=(anywhere, vm, vm),
        scratch_shapes=[B(T, width), B(T, 2 * DH), V(*maps), V(*maps), B(T, width),
                        B(T, 2 * DH), B(T, width), V(T, width), V(T, width), B(T, width), B(T, width), V(T, width),
                        V(tiles, H, DH, 2 * DH), V(H, DH, 2 * DH), V(H, DH, 2 * DH), V(H, DH, DH), V(H, DH, DH),
                        B(H, 2 * DH, DH), B(H, 2 * DH, DH), V(2, size, DH, H * DH // 2),
                        dma((4,)), dma((tiles,)), dma((rows // C, size)), dma((rows // C,)), dma((2, size)), dma((2, size))],
        compiler_params=pltpu.CompilerParams(collective_id=1, has_side_effects=True, vmem_limit_bytes=60 * 2**20),
        cost_estimate=pl.CostEstimate(flops=4 * T * T * width, bytes_accessed=8 * T * width, transcendentals=T * T * H),
    )(q, kv, map_query, map_key)


def project_kernel(chunk, t_hbm, wq_hbm, wk_hbm, wv_hbm, cos_ref, sin_ref, q_out, kv_out,
                   tok, wq, wp, acc, stq, stkv, ssem, rsem, wsem, tsem, qsend, qrecv, ksend, krecv, own_sem):
    size = lax.axis_size("seq")
    me = lax.axis_index("seq")
    place = lax.axis_index("head")
    z, x = place // 2, place % 2
    last = lax.axis_size("head") // 2 - 1
    rows, depth = t_hbm.shape
    width = wq_hbm.shape[1]
    share = width // size
    chunks = rows // chunk
    half = chunks // 2
    above = jnp.minimum(z + 1, last) * 2 + x
    below = jnp.maximum(z - 1, 0) * 2 + x
    beside = z * 2 + 1 - x
    twin = z + 1 - 2 * (z % 2)
    e1 = twin
    e2 = jnp.where(z < 2, 2, 1)
    e3 = jnp.where(z < 2, 3, 0)

    barrier = pltpu.get_barrier_semaphore()
    @pl.when(z < last)
    def _():
        pl.semaphore_signal(barrier, 1, device_id={"head": above}, device_id_type=MESH)
    @pl.when(z > 0)
    def _():
        pl.semaphore_signal(barrier, 1, device_id={"head": below}, device_id_type=MESH)
    pl.semaphore_signal(barrier, 1, device_id={"head": beside}, device_id_type=MESH)
    for shift in range(1, size):
        pl.semaphore_signal(barrier, 1, device_id={"seq": lax.rem(me + shift, size)}, device_id_type=MESH)

    def load(d):
        at = pl.ds(pl.multiple_of(d * depth, depth), depth)
        return (
            pltpu.make_async_copy(wq_hbm.at[at], wq.at[at], wsem.at[0, d]),
            pltpu.make_async_copy(wk_hbm.at[at], wp.at[at, pl.ds(0, DH)], wsem.at[1, d]),
            pltpu.make_async_copy(wv_hbm.at[at], wp.at[at, pl.ds(DH, DH)], wsem.at[2, d]),
        )
    mine = pltpu.make_async_copy(t_hbm, tok.at[place], tsem)
    mine.start()
    order = [place, e1 * 2 + x, z * 2 + 1 - x, e2 * 2 + x, e1 * 2 + 1 - x, e3 * 2 + x, e2 * 2 + 1 - x, e3 * 2 + 1 - x]
    for d in order:
        for copy in load(d):
            copy.start()
    pl.semaphore_wait(barrier, size + jnp.where(z > 0, 1, 0) + jnp.where(z < last, 1, 0))

    def span(c):
        return pl.ds(pl.multiple_of(c * chunk, chunk), chunk)

    def send(c, d, kind, to, own=False):
        return pltpu.make_async_remote_copy(
            src_ref=t_hbm.at[span(c)] if own else tok.at[d, span(c)],
            dst_ref=tok.at[d, span(c)],
            send_sem=ssem.at[c, kind],
            recv_sem=rsem.at[c, d],
            device_id={"head": to},
            device_id_type=MESH,
        )

    def arrived(c, d):
        send(c, d, 0, beside).wait_recv()

    def own_sends(c, act):
        @pl.when(z < last)
        def _():
            act(send(c, place, 0, above, True))
        @pl.when(z > 0)
        def _():
            act(send(c, place, 1, below, True))
        act(send(c, place, 2, beside, True))

    def relays(c, n, e, act):
        d = e * 2 + x
        @pl.when((e > z) & (z > 0))
        def _():
            act(send(c, d, 2 + n, below))
        @pl.when((e < z) & (z < last))
        def _():
            act(send(c, d, 2 + n, above))
        if n == 1:
            @pl.when(c < half)
            def _():
                act(send(c, d, 5 + n, beside))
        else:
            act(send(c, d, 5 + n, beside))

    def twin_sends(act):
        def one(c, carry):
            act(send(c, beside, 9, twin * 2 + x))
            return carry
        lax.fori_loop(half, chunks, one, 0)

    def outputs(c, act, local):
        at = pl.ds(pl.multiple_of(me * rows + c * chunk, chunk), chunk)
        for shift in range(1, size):
            to = lax.rem(me + shift, size)
            act(pltpu.make_async_remote_copy(
                src_ref=stkv.at[c], dst_ref=kv_out.at[at], send_sem=ksend.at[c, shift], recv_sem=krecv.at[c, shift],
                device_id={"seq": to}, device_id_type=MESH))
            act(pltpu.make_async_remote_copy(
                src_ref=stq.at[c, to], dst_ref=q_out.at[at], send_sem=qsend.at[c, shift], recv_sem=qrecv.at[c, shift],
                device_id={"seq": to}, device_id_type=MESH))
        local(pltpu.make_async_copy(stkv.at[c], kv_out.at[at], own_sem.at[c, 0]))
        local(pltpu.make_async_copy(stq.at[c, me], q_out.at[at], own_sem.at[c, 1]))

    start = lambda copy: copy.start()

    def weights_of(d):
        for copy in load(d):
            copy.wait()

    def multiply(row, count, d, first=False):
        at = pl.ds(pl.multiple_of(d * depth, depth), depth)
        to = pl.ds(row, count)
        block = tok[d, to, :]
        for p in range(size):
            cols = slice(p * share, (p + 1) * share)
            v = dot_nn(block, wq[at, cols])
            acc[to, cols] = v if first else acc[to, cols] + v
        v = dot_nn(block, wp[at, :])
        acc[to, width:] = v if first else acc[to, width:] + v

    def each(low, high, body):
        def one(c, carry):
            body(c)
            return carry
        lax.fori_loop(low, high, one, 0)

    each(0, chunks, lambda c: own_sends(c, start))
    mine.wait()
    weights_of(place)
    multiply(0, rows, place, True)
    o1, o2, o3 = e1 * 2 + x, e2 * 2 + x, e3 * 2 + x
    f1, f2, f3 = e1 * 2 + 1 - x, e2 * 2 + 1 - x, e3 * 2 + 1 - x

    def column(n, e, d):
        def body(c):
            arrived(c, d)
            relays(c, n, e, start)
        return body
    each(0, chunks, column(1, e1, o1))
    weights_of(o1)
    multiply(0, rows, o1)
    each(0, chunks, lambda c: arrived(c, beside))
    inner = (z > 0) & (z < last)
    @pl.when(jnp.logical_not(inner))
    def _():
        twin_sends(start)
    weights_of(beside)
    multiply(0, rows, beside)
    each(0, chunks, column(2, e2, o2))
    weights_of(o2)
    multiply(0, rows, o2)
    each(0, half, lambda c: arrived(c, f1))
    weights_of(f1)
    multiply(0, half * chunk, f1)
    weights_of(o3)
    weights_of(f2)
    weights_of(f3)

    def step(k, carry):
        @pl.when(k < chunks)
        def _():
            column(3, e3, o3)(k)
            row = pl.multiple_of(k * chunk, chunk)
            multiply(row, chunk, o3)
            @pl.when((k == chunks - 1) & inner)
            def _():
                twin_sends(start)
            arrived(k, f2)
            multiply(row, chunk, f2)
        @pl.when(k >= half)
        def _():
            c = k - half
            row = pl.multiple_of(c * chunk, chunk)
            @pl.when(c >= half)
            def _():
                arrived(c, f1)
                multiply(row, chunk, f1)
            arrived(c, f3)
            multiply(row, chunk, f3)
            cosine = cos_ref[span(c), :]
            sine = sin_ref[span(c), :]
            rotate_rows = lambda v: (v * cosine + pltpu.roll(v, DH // 2, 1) * sine).astype(BF16)
            per = share // DH
            stkv[c, :, :DH] = rotate_rows(acc[span(c), width:width + DH].astype(BF16).astype(F32))
            stkv[c, :, DH:] = acc[span(c), width + DH:].astype(BF16)
            for p in range(size):
                for h in range(per):
                    at = (p * per + h) * DH
                    stq[c, p, :, h * DH:(h + 1) * DH] = rotate_rows(acc[span(c), at:at + DH])
            outputs(c, start, start)
        return carry
    lax.fori_loop(0, chunks + half, step, 0)

    done = lambda copy: copy.wait_send()
    def finish(c):
        own_sends(c, done)
        for n, e in ((1, e1), (2, e2), (3, e3)):
            relays(c, n, e, done)
        outputs(c, lambda copy: copy.wait(), lambda copy: copy.wait())
    each(0, chunks, finish)
    twin_sends(done)

def project_exchange(tokens, w_query, w_key, w_value, cosine, sine, chunks=8):
    size = lax.axis_size("seq")
    rows, depth = tokens.shape
    full, width = w_query.shape
    share = width // size
    chunk = rows // chunks
    blocks = full // depth
    any_ = pl.BlockSpec(memory_space=pl.ANY)
    vm = pl.BlockSpec(memory_space=pltpu.VMEM)
    dma = pltpu.SemaphoreType.DMA
    return pl.pallas_call(
        functools.partial(project_kernel, chunk),
        out_shape=(jax.ShapeDtypeStruct((rows * size, share), BF16), jax.ShapeDtypeStruct((rows * size, 2 * DH), BF16)),
        in_specs=[any_] * 4 + [vm] * 2,
        out_specs=(any_, any_),
        scratch_shapes=[
            pltpu.VMEM((blocks, rows, depth), BF16),
            pltpu.VMEM((full, width), BF16),
            pltpu.VMEM((full, 2 * DH), BF16),
            pltpu.VMEM((rows, width + 2 * DH), F32),
            pltpu.VMEM((chunks, size, chunk, share), BF16),
            pltpu.VMEM((chunks, chunk, 2 * DH), BF16),
            dma((chunks, 10)), dma((chunks, blocks)), dma((3, blocks)), dma,
            dma((chunks, size)), dma((chunks, size)), dma((chunks, size)), dma((chunks, size)), dma((chunks, 2)),
        ],
        compiler_params=pltpu.CompilerParams(collective_id=0, has_side_effects=True, vmem_limit_bytes=62 * 2**20),
        cost_estimate=pl.CostEstimate(flops=2 * rows * full * (width + 2 * DH), bytes_accessed=full * width * 2, transcendentals=0),
    )(tokens, w_query, w_key, w_value, cosine, sine)


def per_device_by_heads(tokens, w_query, w_key, w_value, map_query, map_key):
    row_count = tokens.shape[0]
    me = lax.axis_index("seq")
    cosine, sine = rope_tables(row_count, DH, me * row_count)
    queries, pair = project_exchange(
        tokens, w_query, w_key, w_value,
        jnp.concatenate([cosine, cosine], 1), jnp.concatenate([-sine, sine], 1),
    )
    return attention(queries, pair, map_query, map_key, row_count)


def fits(mesh, tokens, w_query, w_key):
    heads = w_query.shape[1] // mesh.shape["head"] // DH
    rows = tokens.shape[0] // mesh.shape["seq"]
    return (
        mesh.shape["head"] == 8
        and w_key.shape[1] // mesh.shape["head"] == DH
        and heads % (2 * mesh.shape["seq"]) == 0
        and rows % 256 == 0
    )


def solution(mesh):
    in_specs = (
        P("seq", "head"),
        P(None, "head"),
        P(None, "head"),
        P(None, "head"),
        P("head", None, None),
        P("head", None, None),
    )
    out_specs = (P("seq", "head"), P("head", None, None), P("head", None, None))

    def run(tokens, w_query, w_key, w_value, map_query, map_key):
        body = per_device_by_heads if fits(mesh, tokens, w_query, w_key) else per_device_by_rows
        return jax.shard_map(
            body, mesh=mesh, in_specs=in_specs, out_specs=out_specs, check_vma=False
        )(tokens, w_query, w_key, w_value, map_query, map_key)

    return run
```

```python
import functools
import math

import jax
import jax.numpy as jnp
from jax import lax
from jax.experimental import pallas as pl
from jax.experimental.pallas import tpu as pltpu
from jax.sharding import PartitionSpec as P

DH = 128


ROPE_BASE = 500000.0
MATMUL_ACCURACY = lax.Precision.DEFAULT


def partner(value, axis, apart):
    mask = 2**apart
    pairs = [(source, source ^ mask) for source in range(lax.axis_size(axis))]
    return lax.ppermute(value, axis, pairs)


def rope_tables(length, width, offset):
    half_width = width // 2
    positions = (offset + jnp.arange(length)).astype(jnp.float32)
    exponent = jnp.arange(half_width).astype(jnp.float32) * (2.0 / width)
    frequency = jnp.power(jnp.float32(ROPE_BASE), -exponent)
    angles = positions[:, None] * frequency[None, :]
    return (jnp.cos(angles), jnp.sin(angles))


def rotate(vectors, cosine, sine):
    half_width = vectors.shape[-1] // 2
    first = vectors[..., :half_width]
    second = vectors[..., half_width:]
    cosine = cosine[:, None, :]
    sine = sine[:, None, :]
    return jnp.concatenate(
        [first * cosine - second * sine, second * cosine + first * sine], axis=-1
    )


def feature_map(vectors, weights):
    logits = jnp.einsum("thd,hdf->thf", vectors, weights, precision=MATMUL_ACCURACY)
    upper = jnp.exp(logits)
    lower = jnp.exp(-logits)
    return jnp.concatenate(
        [upper / jnp.sum(upper, -1, keepdims=True), lower / jnp.sum(lower, -1, keepdims=True)],
        axis=-1,
    )


def teacher_kernel(first_ref, query_ref, key_ref, value_ref, out_ref):
    rows = query_ref.shape[0]
    block = rows // 2 if rows % 2 == 0 else rows
    first = first_ref[0]
    scale = 1.0 / math.sqrt(query_ref.shape[1])
    queries = query_ref[...]

    def scored(start):
        keys = key_ref[pl.ds(start, block), :]
        scores = lax.dot_general(
            queries, keys, (((1,), (1,)), ((), ())), preferred_element_type=jnp.float32
        )
        return scores * scale

    def add(carry, weights, start):
        numerator, denominator = carry
        values = value_ref[pl.ds(start, block), :]
        denominator = denominator + jnp.sum(weights, axis=1, keepdims=True)
        numerator = numerator + jnp.dot(
            weights.astype(jnp.bfloat16), values, preferred_element_type=jnp.float32
        )
        return numerator, denominator

    def earlier(index, carry):
        start = pl.multiple_of(index * block, block)
        return add(carry, jnp.exp(scored(start)), start)

    carry = (
        jnp.zeros((rows, out_ref.shape[1]), jnp.float32),
        jnp.zeros((rows, 1), jnp.float32),
    )
    carry = lax.fori_loop(0, first // block, earlier, carry)
    for part in range(rows // block):
        start = pl.multiple_of(first + part * block, block)
        row = lax.broadcasted_iota(jnp.int32, (rows, block), 0)
        column = lax.broadcasted_iota(jnp.int32, (rows, block), 1) + part * block
        weights = jnp.exp(jnp.where(column <= row, scored(start), -1e30))
        carry = add(carry, weights, start)
    numerator, denominator = carry
    out_ref[...] = (numerator / denominator).astype(out_ref.dtype)


def teacher_attention(first, queries_rot, keys_rot, values):
    rows, width = queries_rot.shape
    span = keys_rot.shape[0]
    return pl.pallas_call(
        teacher_kernel,
        out_shape=jax.ShapeDtypeStruct((rows, width), jnp.bfloat16),
        grid_spec=pltpu.PrefetchScalarGridSpec(
            num_scalar_prefetch=1,
            grid=(width // DH,),
            in_specs=[
                pl.BlockSpec((rows, DH), lambda head, first: (0, head)),
                pl.BlockSpec((span, DH), lambda head, first: (0, 0)),
                pl.BlockSpec((span, DH), lambda head, first: (0, 0)),
            ],
            out_specs=pl.BlockSpec((rows, DH), lambda head, first: (0, head)),
        ),
        compiler_params=pltpu.CompilerParams(vmem_limit_bytes=32 * 1024 * 1024),
        cost_estimate=pl.CostEstimate(
            flops=4 * rows * span * width,
            bytes_accessed=4 * rows * width + 4 * span * DH,
            transcendentals=rows * span * (width // DH),
        ),
    )(jnp.reshape(first, (1,)).astype(jnp.int32), queries_rot, keys_rot, values)


def from_lower(value, shift):
    size = lax.axis_size("seq")
    return lax.ppermute(value, "seq", [(i, i + shift) for i in range(size - shift)])


def from_higher(value, shift):
    size = lax.axis_size("seq")
    return lax.ppermute(value, "seq", [(i + shift, i) for i in range(size - shift)])


def sum_of_others(arrays, receive):
    totals = [jnp.zeros(array.shape, jnp.float32) for array in arrays]
    for shift in range(1, lax.axis_size("seq")):
        for slot, array in enumerate(arrays):
            totals[slot] = totals[slot] + receive(array, shift).astype(jnp.float32)
    return totals


def gather_seq(piece):
    size = lax.axis_size("seq")
    rows = piece.shape[0]
    me = lax.axis_index("seq")
    whole = jnp.zeros((size * rows,) + piece.shape[1:], piece.dtype)
    whole = lax.dynamic_update_slice_in_dim(whole, piece, me * rows, 0)
    for shift in range(1, size):
        source = (me - shift + size) % size
        got = lax.ppermute(piece, "seq", [(i, (i + shift) % size) for i in range(size)])
        whole = lax.dynamic_update_slice_in_dim(whole, got, source * rows, 0)
    return whole


def token_blocks(tokens):
    size = lax.axis_size("head")
    me = lax.axis_index("head")
    if size != 8:
        gathered = lax.all_gather(tokens, "head", axis=1, tiled=True)
        return [(jnp.int32(0), gathered)]
    ring = size // 2
    z, x = me // 2, me % 2

    def up(value):
        return lax.ppermute(value, "head", [(s, (s + 2) % size) for s in range(size)])

    def down(value):
        return lax.ppermute(value, "head", [(s, (s + size - 2) % size) for s in range(size)])

    def across(value):
        return lax.ppermute(value, "head", [(s, s ^ 1) for s in range(size)])

    def index(dz, dx):
        return ((z + dz) % ring) * 2 + (x + dx) % 2

    half = tokens.shape[0] // 2
    below = up(tokens)
    above = down(tokens)
    beside = across(tokens)
    far = jnp.concatenate([up(below[:half]), down(above[half:])], 0)
    beside_below = up(beside)
    beside_above = down(beside)
    beside_far = across(far)
    return [
        (index(0, 0), tokens),
        (index(0, 1), beside),
        (index(ring - 1, 0), below),
        (index(1, 0), above),
        (index(2, 0), far),
        (index(ring - 1, 1), beside_below),
        (index(1, 1), beside_above),
        (index(2, 1), beside_far),
    ]


def per_device_by_rows(tokens, w_query, w_key, w_value, map_query, map_key):
    row_count = tokens.shape[0]
    head_count = w_query.shape[1] // DH
    shared_width = w_key.shape[1]
    w_pair = jnp.concatenate([w_key, w_value], 1)
    query_rows = jnp.zeros((row_count, w_query.shape[1]), jnp.float32)
    pair_rows = jnp.zeros((row_count, w_pair.shape[1]), jnp.float32)
    for position, block in token_blocks(tokens):
        depth = block.shape[1]
        weights = lax.dynamic_slice_in_dim(w_query, position * depth, depth, 0)
        pair_weights = lax.dynamic_slice_in_dim(w_pair, position * depth, depth, 0)
        query_rows = query_rows + jnp.dot(block, weights, preferred_element_type=jnp.float32)
        pair_rows = pair_rows + jnp.dot(block, pair_weights, preferred_element_type=jnp.float32)
    keys = pair_rows[:, :shared_width]
    values = pair_rows[:, shared_width:]
    keys = keys.astype(jnp.bfloat16)
    values = values.astype(jnp.bfloat16)
    if shared_width < DH:
        partner_keys, partner_values = partner((keys, values), "head", 0)
        upper_half = lax.axis_index("head") % 2 == 1
        keys = jnp.where(
            upper_half,
            jnp.concatenate([partner_keys, keys], 1),
            jnp.concatenate([keys, partner_keys], 1),
        )
        values = jnp.where(
            upper_half,
            jnp.concatenate([partner_values, values], 1),
            jnp.concatenate([values, partner_values], 1),
        )
    chain_index = lax.axis_index("seq")
    query_first = chain_index * row_count
    cosine, sine = rope_tables(row_count, DH, query_first)
    queries_rot = rotate(query_rows.reshape(row_count, head_count, DH), cosine, sine).astype(
        jnp.bfloat16
    )
    keys_rot = (
        rotate(keys.astype(jnp.float32).reshape(row_count, 1, DH), cosine, sine)
        .reshape(row_count, DH)
        .astype(jnp.bfloat16)
    )
    pair_all = gather_seq(jnp.concatenate([keys_rot, values], 1))
    teacher = teacher_attention(
        query_first,
        queries_rot.reshape(row_count, head_count * DH),
        pair_all[:, :DH],
        pair_all[:, DH:],
    )
    query_float = queries_rot.astype(jnp.float32)
    key_float = jnp.broadcast_to(
        keys_rot.astype(jnp.float32)[:, None, :], (row_count, head_count, DH)
    )
    value_single_float = values.astype(jnp.float32)
    query_features = feature_map(query_float, map_query)
    key_features = feature_map(key_float, map_key)
    state_local = jnp.einsum(
        "thf,td->hfd", key_features, value_single_float, precision=MATMUL_ACCURACY
    )
    norm_local = jnp.sum(key_features, 0)
    state_before, norm_before = sum_of_others(
        (state_local.astype(jnp.bfloat16), norm_local), from_lower
    )
    local_mask = (jnp.arange(row_count)[None, :] <= jnp.arange(row_count)[:, None]).astype(
        jnp.float32
    )

    def student_local(query_feature_rows, key_feature_rows, state, norm):
        within = (
            jnp.einsum(
                "ueo,aeo->eua", query_feature_rows, key_feature_rows, precision=MATMUL_ACCURACY
            )
            * local_mask[None]
        )
        upper = jnp.einsum("hqk,kd->qhd", within, value_single_float, precision=MATMUL_ACCURACY)
        upper = upper + jnp.einsum(
            "qhf,hfd->qhd", query_feature_rows, state, precision=MATMUL_ACCURACY
        )
        lower = jnp.transpose(jnp.sum(within, -1)) + jnp.einsum(
            "qhf,hf->qh", query_feature_rows, norm, precision=MATMUL_ACCURACY
        )
        return upper / lower[..., None]

    student, pullback = jax.vjp(
        student_local, query_features, key_features, state_before, norm_before
    )
    student_out = student.astype(jnp.bfloat16).reshape(row_count, head_count * DH)
    target = teacher.reshape(row_count, head_count, DH).astype(jnp.float32)
    grad_student = 2.0 * (student - target)
    grad_query_feat, grad_key_feat, grad_state, grad_norm = pullback(grad_student)
    state_after, norm_after = sum_of_others(
        (grad_state.astype(jnp.bfloat16), grad_norm), from_higher
    )
    grad_key_feat = (
        grad_key_feat
        + jnp.einsum("td,hfd->thf", value_single_float, state_after, precision=MATMUL_ACCURACY)
        + norm_after[None]
    )
    unused_query, query_backward = jax.vjp(
        lambda weights: feature_map(query_float, weights), map_query
    )
    unused_key, pull_key = jax.vjp(lambda weights: feature_map(key_float, weights), map_key)
    grad_query = query_backward(grad_query_feat)[0]
    grad_key = pull_key(grad_key_feat)[0]
    features = grad_query.shape[-1]
    grads = jnp.concatenate([grad_query, grad_key], -1)
    size = lax.axis_size("seq")
    if size & (size - 1):
        grads = lax.psum(grads, "seq")
    else:
        apart = 0
        while 2**apart < size:
            if apart > 0:
                sent = grads.astype(jnp.bfloat16)
                grads = sent.astype(jnp.float32) + partner(sent, "seq", apart).astype(jnp.float32)
            else:
                grads = grads + partner(grads, "seq", apart)
            apart += 1
    grad_query, grad_key = grads[..., :features], grads[..., features:]
    return (student_out, grad_query, grad_key)


F32 = jnp.float32
BF16 = jnp.bfloat16
MESH = pl.DeviceIdType.MESH


def dot_nn(a, b):
    return lax.dot_general(a, b, (((1,), (0,)), ((), ())), preferred_element_type=F32)
def dot_nt(a, b):
    return lax.dot_general(a, b, (((1,), (1,)), ((), ())), preferred_element_type=F32)
def dot_tn(a, b):
    return lax.dot_general(a, b, (((0,), (0,)), ((), ())), preferred_element_type=F32)

def split(v):
    high = v.astype(BF16)
    low = (v - high.astype(F32)).astype(BF16)
    return high, low

def half_sums(v, ones):
    high, low = split(v)
    return dot_nn(jnp.concatenate([high, low], 1), ones)

def attention_kernel(C, q_hbm, kv_hbm, mapq_hbm, mapk_hbm, out_hbm, gradq_ref, gradk_ref,
                     q_ref, kv_ref, mq_ref, mk_ref, out_ref, vaug, tch, qf, kf, qfb, kfb, dk, gu, state, gsum, mq, mk,
                     wq, wk, land, load_sem, out_send, out_recv, own_sem, grad_send, grad_recv):
    T = q_ref.shape[0]
    W = out_hbm.shape[0]
    size = lax.axis_size("seq")
    me = lax.axis_index("seq")
    barrier = pltpu.get_barrier_semaphore()
    for shift in range(1, size):
        pl.semaphore_signal(barrier, 1, device_id={"seq": lax.rem(me + shift, size)}, device_id_type=MESH)
    heads_here = pl.ds(me * (q_ref.shape[1] // DH), q_ref.shape[1] // DH)
    loads = [pltpu.make_async_copy(src, dst, load_sem.at[n]) for n, (src, dst) in enumerate((
        (mapq_hbm.at[heads_here], mq_ref), (mapk_hbm.at[heads_here], mk_ref), (kv_hbm, kv_ref), (q_hbm, q_ref)))]
    for copy in loads:
        copy.start()
    pl.semaphore_wait(barrier, size - 1)
    for copy in loads:
        copy.wait()
    H = q_ref.shape[1] // DH
    tiles = T // C
    scale = math.log2(math.e) / math.sqrt(DH)
    r = lax.broadcasted_iota(jnp.int32, (2 * DH, DH), 0)
    c = lax.broadcasted_iota(jnp.int32, (2 * DH, DH), 1)
    half = DH // 2
    ones = jnp.where((r % DH) // half == c // half, 1.0, 0.0).astype(BF16)
    row = lax.broadcasted_iota(jnp.int32, (C, C), 0)
    column = lax.broadcasted_iota(jnp.int32, (C, C), 1)
    causal = column <= row
    for h in range(H):
        for src, dst in ((mq_ref, wq), (mk_ref, wk)):
            w = src[h].T
            high, low = split(jnp.concatenate([w, -w], 1))
            dst[h] = jnp.concatenate([high, low], 0)
    state[...] = jnp.zeros_like(state)
    gsum[...] = jnp.zeros_like(gsum)
    mq[...] = jnp.zeros_like(mq)
    mk[...] = jnp.zeros_like(mk)

    def rows_of(i):
        return pl.ds(pl.multiple_of(i * C, C), C)

    def features(i, carry):
        rows = rows_of(i)
        k = kv_ref[rows, :DH]
        vaug[rows, :DH] = kv_ref[rows, DH:]
        vaug[rows, DH:] = jnp.ones((C, DH), BF16)
        k2 = jnp.concatenate([k, k], 1)
        for h in range(H):
            cols = slice(h * DH, (h + 1) * DH)
            q = q_ref[rows, cols]
            for x2, w, f, fb in ((jnp.concatenate([q, q], 1), wq, qf, qfb), (k2, wk, kf, kfb)):
                e = jnp.exp(dot_nn(x2, w[h]))
                phi = e / half_sums(e, ones)
                f[rows, cols] = phi
                fb[rows, cols] = phi.astype(BF16)
        return carry
    lax.fori_loop(0, tiles, features, 0, unroll=2)

    def phi_back(phi, d):
        return (phi * (d - half_sums(d * phi, ones))).astype(BF16)

    big = W // C
    heads = range(H)
    width = H * DH

    def out_copy(i, local):
        owner = i // big
        to = out_hbm.at[pl.ds(pl.multiple_of(lax.rem(i, big) * C, C), C), pl.ds(pl.multiple_of(me * width, width), width)]
        if local:
            return pltpu.make_async_copy(out_ref.at[rows_of(i)], to, own_sem.at[lax.rem(i, big)])
        return pltpu.make_async_remote_copy(
            src_ref=out_ref.at[rows_of(i)], dst_ref=to, send_sem=out_send.at[i], recv_sem=out_recv.at[lax.rem(i, big), me],
            device_id={"seq": owner}, device_id_type=MESH)

    def give(i, act_local, act_remote):
        @pl.when(i // big == me)
        def _():
            act_local(out_copy(i, True))
        @pl.when(i // big != me)
        def _():
            act_remote(out_copy(i, False))

    start = lambda copy: copy.start()

    def grad_copy(kind, shift):
        return pltpu.make_async_remote_copy(
            src_ref=land.at[kind, me], dst_ref=land.at[kind, me], send_sem=grad_send.at[kind, shift],
            recv_sem=grad_recv.at[kind, shift], device_id={"seq": lax.rem(me + shift, size)}, device_id_type=MESH)

    def give_grads(kind, total):
        for h in heads:
            v = total[h]
            land[kind, me, h] = (v[:, :half] - v[:, half:]).T
        for shift in range(1, size):
            grad_copy(kind, shift).start()

    def teach(n, carry):
        first = n * big
        rows = pl.ds(pl.multiple_of(n * W, W), W)
        q = jnp.concatenate([q_ref[rows, h * DH:(h + 1) * DH] for h in heads], 0)

        def earlier(j, acc):
            seen = pl.ds(pl.multiple_of(j * W, W), W)
            s = dot_nt(q, kv_ref[seen, :DH]) * scale
            return acc + dot_nn(jnp.exp2(s).astype(BF16), vaug[seen, :])
        acc = lax.fori_loop(0, n, earlier, jnp.zeros((H * W, 2 * DH), F32))
        parts = []
        for b in range(big):
            seen = pl.ds(pl.multiple_of(n * W + b * C, C), C)
            q = jnp.concatenate([q_ref[pl.ds(pl.multiple_of(n * W + b * C, C), W - b * C), h * DH:(h + 1) * DH] for h in heads], 0)
            s = dot_nt(q, kv_ref[seen, :DH]) * scale
            left = W - b * C
            s = jnp.concatenate([x for h in heads for x in
                                 [jnp.where(causal, s[h * left:h * left + C], -1e30), s[h * left + C:(h + 1) * left]]], 0) if left > C else jnp.concatenate([jnp.where(causal, s[h * C:(h + 1) * C], -1e30) for h in heads], 0)
            p = dot_nn(jnp.exp2(s).astype(BF16), vaug[seen, :])
            parts.append(p)
        for h in heads:
            for b in range(big):
                v = acc[h * W + b * C:h * W + (b + 1) * C]
                for b2 in range(b + 1):
                    left = W - b2 * C
                    lo = h * left + (b - b2) * C
                    v = v + parts[b2][lo:lo + C]
                tch[pl.ds(pl.multiple_of(n * W + b * C, C), C), h * DH:(h + 1) * DH] = (v[:, :DH] / v[:, DH:]).astype(BF16)
        return carry
    lax.fori_loop(0, T // W, teach, 0)

    def forward(i, carry):
        @pl.when(i > 0)
        def _():
            give(i - 1, start, start)
        rows = rows_of(i)
        va = vaug[rows, :]
        cols = [slice(h * DH, (h + 1) * DH) for h in heads]
        fq = [qfb[rows, cols[h]] for h in heads]
        fk = [kfb[rows, cols[h]] for h in heads]
        st = [state[h] for h in heads]
        stb = [x.astype(BF16) for x in st]
        a = [jnp.where(causal, dot_nt(fq[h], fk[h]), 0.0).astype(BF16) for h in heads]
        av = dot_nn(jnp.concatenate(a, 0), va)
        dua = []
        for h in heads:
            nd = av[h * C:(h + 1) * C] + dot_nn(fq[h], stb[h])
            inv = 1.0 / nd[:, DH:]
            y = nd[:, :DH] * inv
            out_ref[rows, cols[h]] = y.astype(out_ref.dtype)
            du = ((2.0 * (y - tch[rows, cols[h]].astype(F32))) * inv).astype(BF16)
            dl = jnp.sum(du.astype(F32) * y, 1, keepdims=True) * (-1.0 / half)
            dl_high, dl_low = split(dl)
            dua.append(jnp.concatenate([du, jnp.broadcast_to(dl_high, (C, half)), jnp.broadcast_to(dl_low, (C, half))], 1))
            state[h] = st[h] + dot_tn(fk[h], va)
        dall = dot_nt(jnp.concatenate(dua, 0), va)
        for h in heads:
            da = jnp.where(causal, dall[h * C:(h + 1) * C], 0.0).astype(BF16)
            dq = dot_nn(da, fk[h]) + dot_nt(dua[h], stb[h])
            dk[rows, cols[h]] = dot_tn(da, fq[h])
            gu[i, h] = dot_tn(fq[h], dua[h])
            g = phi_back(qf[rows, cols[h]], dq)
            mq[h] += dot_tn(q_ref[rows, cols[h]], g)
        return carry
    lax.fori_loop(0, tiles, forward, 0, unroll=2)
    give(tiles - 1, start, start)
    give_grads(0, mq)

    def backward(n, carry):
        i = tiles - 1 - n
        rows = rows_of(i)
        va = vaug[rows, :]
        keys = kv_ref[rows, :DH]
        for h in range(H):
            cols = slice(h * DH, (h + 1) * DH)
            d = dk[rows, cols] + dot_nt(va, gsum[h].astype(BF16))
            g = phi_back(kf[rows, cols], d)
            mk[h] += dot_tn(keys, g)
            gsum[h] += gu[i, h]
        return carry
    lax.fori_loop(0, tiles, backward, 0, unroll=2)
    give_grads(1, mk)

    def finish(i, carry):
        give(i, lambda copy: copy.wait(), lambda copy: copy.wait_send())
        return carry
    lax.fori_loop(0, tiles, finish, 0)
    for b in range(big):
        for shift in range(1, size):
            source = lax.rem(me + shift, size)
            pltpu.make_async_remote_copy(
                src_ref=out_ref.at[rows_of(b)],
                dst_ref=out_hbm.at[pl.ds(b * C, C), pl.ds(pl.multiple_of(source * width, width), width)],
                send_sem=out_send.at[b], recv_sem=out_recv.at[b, source],
                device_id={"seq": source}, device_id_type=MESH).wait_recv()
    for kind, ref in ((0, gradq_ref), (1, gradk_ref)):
        for shift in range(1, size):
            grad_copy(kind, shift).wait()
        for n in range(size):
            for h in heads:
                ref[n * H + h] = land[kind, n, h]


def attention(q, kv, map_query, map_key, rows, C=256):
    T, width = q.shape
    H = width // DH
    count = map_query.shape[0]
    map_query, map_key = jnp.swapaxes(map_query, 1, 2), jnp.swapaxes(map_key, 1, 2)
    size = lax.axis_size("seq")
    V = lambda *s: pltpu.VMEM(s, F32)
    B = lambda *s: pltpu.VMEM(s, BF16)
    dma = pltpu.SemaphoreType.DMA
    vm = pl.BlockSpec(memory_space=pltpu.VMEM)
    anywhere = pl.BlockSpec(memory_space=pl.ANY)
    grads = jax.ShapeDtypeStruct(map_query.shape, F32)
    maps = (H,) + map_query.shape[1:]
    tiles = T // C
    out, grad_query, grad_key = pl.pallas_call(
        functools.partial(attention_kernel, C),
        out_shape=(jax.ShapeDtypeStruct((rows, count * DH), BF16), grads, grads),
        in_specs=[anywhere] * 4,
        out_specs=(anywhere, vm, vm),
        scratch_shapes=[B(T, width), B(T, 2 * DH), V(*maps), V(*maps), B(T, width),
                        B(T, 2 * DH), B(T, width), V(T, width), V(T, width), B(T, width), B(T, width), V(T, width),
                        V(tiles, H, DH, 2 * DH), V(H, DH, 2 * DH), V(H, DH, 2 * DH), V(H, DH, DH), V(H, DH, DH),
                        B(H, 2 * DH, DH), B(H, 2 * DH, DH), V(2, size, H, DH // 2, DH),
                        dma((4,)), dma((tiles,)), dma((rows // C, size)), dma((rows // C,)), dma((2, size)), dma((2, size))],
        compiler_params=pltpu.CompilerParams(collective_id=1, has_side_effects=True, vmem_limit_bytes=60 * 2**20),
        cost_estimate=pl.CostEstimate(flops=4 * T * T * width, bytes_accessed=8 * T * width, transcendentals=T * T * H),
    )(q, kv, map_query, map_key)
    return out, jnp.swapaxes(grad_query, 1, 2), jnp.swapaxes(grad_key, 1, 2)


def project_kernel(chunk, t_hbm, wq_hbm, wk_hbm, wv_hbm, cos_ref, sin_ref, q_out, kv_out,
                   tok, wq, wp, acc, stq, stkv, ssem, rsem, wsem, tsem, qsend, qrecv, ksend, krecv, own_sem):
    size = lax.axis_size("seq")
    me = lax.axis_index("seq")
    place = lax.axis_index("head")
    z, x = place // 2, place % 2
    last = lax.axis_size("head") // 2 - 1
    rows, depth = t_hbm.shape
    width = wq_hbm.shape[1]
    share = width // size
    chunks = rows // chunk
    half = chunks // 2
    above = jnp.minimum(z + 1, last) * 2 + x
    below = jnp.maximum(z - 1, 0) * 2 + x
    beside = z * 2 + 1 - x
    twin = z + 1 - 2 * (z % 2)
    e1 = twin
    e2 = jnp.where(z < 2, 2, 1)
    e3 = jnp.where(z < 2, 3, 0)

    barrier = pltpu.get_barrier_semaphore()
    @pl.when(z < last)
    def _():
        pl.semaphore_signal(barrier, 1, device_id={"head": above}, device_id_type=MESH)
    @pl.when(z > 0)
    def _():
        pl.semaphore_signal(barrier, 1, device_id={"head": below}, device_id_type=MESH)
    pl.semaphore_signal(barrier, 1, device_id={"head": beside}, device_id_type=MESH)
    for shift in range(1, size):
        pl.semaphore_signal(barrier, 1, device_id={"seq": lax.rem(me + shift, size)}, device_id_type=MESH)

    def load(d):
        at = pl.ds(pl.multiple_of(d * depth, depth), depth)
        return (
            pltpu.make_async_copy(wq_hbm.at[at], wq.at[at], wsem.at[0, d]),
            pltpu.make_async_copy(wk_hbm.at[at], wp.at[at, pl.ds(0, DH)], wsem.at[1, d]),
            pltpu.make_async_copy(wv_hbm.at[at], wp.at[at, pl.ds(DH, DH)], wsem.at[2, d]),
        )
    mine = pltpu.make_async_copy(t_hbm, tok.at[place], tsem)
    mine.start()
    order = [place, e1 * 2 + x, z * 2 + 1 - x, e2 * 2 + x, e1 * 2 + 1 - x, e3 * 2 + x, e2 * 2 + 1 - x, e3 * 2 + 1 - x]
    for d in order:
        for copy in load(d):
            copy.start()
    pl.semaphore_wait(barrier, size + jnp.where(z > 0, 1, 0) + jnp.where(z < last, 1, 0))

    def span(c):
        return pl.ds(pl.multiple_of(c * chunk, chunk), chunk)

    def send(c, d, kind, to, own=False):
        return pltpu.make_async_remote_copy(
            src_ref=t_hbm.at[span(c)] if own else tok.at[d, span(c)],
            dst_ref=tok.at[d, span(c)],
            send_sem=ssem.at[c, kind],
            recv_sem=rsem.at[c, d],
            device_id={"head": to},
            device_id_type=MESH,
        )

    def arrived(c, d):
        send(c, d, 0, beside).wait_recv()

    def own_sends(c, act):
        @pl.when(z < last)
        def _():
            act(send(c, place, 0, above, True))
        @pl.when(z > 0)
        def _():
            act(send(c, place, 1, below, True))
        act(send(c, place, 2, beside, True))

    def relays(c, n, e, act):
        d = e * 2 + x
        @pl.when((e > z) & (z > 0))
        def _():
            act(send(c, d, 2 + n, below))
        @pl.when((e < z) & (z < last))
        def _():
            act(send(c, d, 2 + n, above))
        if n == 1:
            @pl.when(c < half)
            def _():
                act(send(c, d, 5 + n, beside))
        else:
            act(send(c, d, 5 + n, beside))

    def twin_sends(act):
        def one(c, carry):
            act(send(c, beside, 9, twin * 2 + x))
            return carry
        lax.fori_loop(half, chunks, one, 0)

    def outputs(c, act, local):
        at = pl.ds(pl.multiple_of(me * rows + c * chunk, chunk), chunk)
        for shift in range(1, size):
            to = lax.rem(me + shift, size)
            act(pltpu.make_async_remote_copy(
                src_ref=stkv.at[c], dst_ref=kv_out.at[at], send_sem=ksend.at[c, shift], recv_sem=krecv.at[c, shift],
                device_id={"seq": to}, device_id_type=MESH))
            act(pltpu.make_async_remote_copy(
                src_ref=stq.at[c, to], dst_ref=q_out.at[at], send_sem=qsend.at[c, shift], recv_sem=qrecv.at[c, shift],
                device_id={"seq": to}, device_id_type=MESH))
        local(pltpu.make_async_copy(stkv.at[c], kv_out.at[at], own_sem.at[c, 0]))
        local(pltpu.make_async_copy(stq.at[c, me], q_out.at[at], own_sem.at[c, 1]))

    start = lambda copy: copy.start()

    def weights_of(d):
        for copy in load(d):
            copy.wait()

    def multiply(row, count, d, first=False):
        at = pl.ds(pl.multiple_of(d * depth, depth), depth)
        to = pl.ds(row, count)
        block = tok[d, to, :]
        for p in range(size):
            cols = slice(p * share, (p + 1) * share)
            v = dot_nn(block, wq[at, cols])
            acc[to, cols] = v if first else acc[to, cols] + v
        v = dot_nn(block, wp[at, :])
        acc[to, width:] = v if first else acc[to, width:] + v

    def each(low, high, body):
        def one(c, carry):
            body(c)
            return carry
        lax.fori_loop(low, high, one, 0)

    each(0, chunks, lambda c: own_sends(c, start))
    mine.wait()
    weights_of(place)
    multiply(0, rows, place, True)
    o1, o2, o3 = e1 * 2 + x, e2 * 2 + x, e3 * 2 + x
    f1, f2, f3 = e1 * 2 + 1 - x, e2 * 2 + 1 - x, e3 * 2 + 1 - x

    def column(n, e, d):
        def body(c):
            arrived(c, d)
            relays(c, n, e, start)
        return body
    each(0, chunks, column(1, e1, o1))
    weights_of(o1)
    multiply(0, rows, o1)
    each(0, chunks, lambda c: arrived(c, beside))
    inner = (z > 0) & (z < last)
    @pl.when(jnp.logical_not(inner))
    def _():
        twin_sends(start)
    weights_of(beside)
    multiply(0, rows, beside)
    each(0, chunks, column(2, e2, o2))
    weights_of(o2)
    multiply(0, rows, o2)
    each(0, half, lambda c: arrived(c, f1))
    weights_of(f1)
    multiply(0, half * chunk, f1)
    weights_of(o3)
    weights_of(f2)
    weights_of(f3)

    def step(k, carry):
        @pl.when(k < chunks)
        def _():
            column(3, e3, o3)(k)
            row = pl.multiple_of(k * chunk, chunk)
            multiply(row, chunk, o3)
            @pl.when((k == chunks - 1) & inner)
            def _():
                twin_sends(start)
            arrived(k, f2)
            multiply(row, chunk, f2)
        @pl.when(k >= half)
        def _():
            c = k - half
            row = pl.multiple_of(c * chunk, chunk)
            @pl.when(c >= half)
            def _():
                arrived(c, f1)
                multiply(row, chunk, f1)
            arrived(c, f3)
            multiply(row, chunk, f3)
            cosine = jnp.concatenate([cos_ref[span(c), :]] * 2, 1)
            sine = jnp.concatenate([-sin_ref[span(c), :], sin_ref[span(c), :]], 1)
            rotate_rows = lambda v: (v * cosine + pltpu.roll(v, DH // 2, 1) * sine).astype(BF16)
            per = share // DH
            stkv[c, :, :DH] = rotate_rows(acc[span(c), width:width + DH].astype(BF16).astype(F32))
            stkv[c, :, DH:] = acc[span(c), width + DH:].astype(BF16)
            for p in range(size):
                for h in range(per):
                    at = (p * per + h) * DH
                    stq[c, p, :, h * DH:(h + 1) * DH] = rotate_rows(acc[span(c), at:at + DH])
            outputs(c, start, start)
        return carry
    lax.fori_loop(0, chunks + half, step, 0)

    done = lambda copy: copy.wait_send()
    def finish(c):
        own_sends(c, done)
        for n, e in ((1, e1), (2, e2), (3, e3)):
            relays(c, n, e, done)
        outputs(c, lambda copy: copy.wait(), lambda copy: copy.wait())
    each(0, chunks, finish)
    twin_sends(done)

def project_exchange(tokens, w_query, w_key, w_value, cosine, sine, chunks=8):
    size = lax.axis_size("seq")
    rows, depth = tokens.shape
    full, width = w_query.shape
    share = width // size
    chunk = rows // chunks
    blocks = full // depth
    any_ = pl.BlockSpec(memory_space=pl.ANY)
    vm = pl.BlockSpec(memory_space=pltpu.VMEM)
    dma = pltpu.SemaphoreType.DMA
    return pl.pallas_call(
        functools.partial(project_kernel, chunk),
        out_shape=(jax.ShapeDtypeStruct((rows * size, share), BF16), jax.ShapeDtypeStruct((rows * size, 2 * DH), BF16)),
        in_specs=[any_] * 4 + [vm] * 2,
        out_specs=(any_, any_),
        scratch_shapes=[
            pltpu.VMEM((blocks, rows, depth), BF16),
            pltpu.VMEM((full, width), BF16),
            pltpu.VMEM((full, 2 * DH), BF16),
            pltpu.VMEM((rows, width + 2 * DH), F32),
            pltpu.VMEM((chunks, size, chunk, share), BF16),
            pltpu.VMEM((chunks, chunk, 2 * DH), BF16),
            dma((chunks, 10)), dma((chunks, blocks)), dma((3, blocks)), dma,
            dma((chunks, size)), dma((chunks, size)), dma((chunks, size)), dma((chunks, size)), dma((chunks, 2)),
        ],
        compiler_params=pltpu.CompilerParams(collective_id=0, has_side_effects=True, vmem_limit_bytes=62 * 2**20),
        cost_estimate=pl.CostEstimate(flops=2 * rows * full * (width + 2 * DH), bytes_accessed=full * width * 2, transcendentals=0),
    )(tokens, w_query, w_key, w_value, cosine, sine)


def per_device_by_heads(tokens, w_query, w_key, w_value, map_query, map_key):
    row_count = tokens.shape[0]
    me = lax.axis_index("seq")
    cosine, sine = rope_tables(row_count, DH, me * row_count)
    queries, pair = project_exchange(tokens, w_query, w_key, w_value, cosine, sine)
    return attention(queries, pair, map_query, map_key, row_count)


def fits(mesh, tokens, w_query, w_key):
    heads = w_query.shape[1] // mesh.shape["head"] // DH
    rows = tokens.shape[0] // mesh.shape["seq"]
    return (
        mesh.shape["head"] == 8
        and w_key.shape[1] // mesh.shape["head"] == DH
        and heads % mesh.shape["seq"] == 0
        and rows % 256 == 0
    )


def solution(mesh):
    in_specs = (
        P("seq", "head"),
        P(None, "head"),
        P(None, "head"),
        P(None, "head"),
        P("head", None, None),
        P("head", None, None),
    )
    out_specs = (P("seq", "head"), P("head", None, None), P("head", None, None))

    def run(tokens, w_query, w_key, w_value, map_query, map_key):
        body = per_device_by_heads if fits(mesh, tokens, w_query, w_key) else per_device_by_rows
        return jax.shard_map(
            body, mesh=mesh, in_specs=in_specs, out_specs=out_specs, check_vma=False
        )(tokens, w_query, w_key, w_value, map_query, map_key)

    return run
```

```python
import functools
import math

import jax
import jax.numpy as jnp
import numpy as np
from jax import lax
from jax.experimental import pallas as pl
from jax.experimental.pallas import tpu as pltpu
from jax.sharding import PartitionSpec as P

DH = 128


ROPE_BASE = 500000.0
MATMUL_ACCURACY = lax.Precision.DEFAULT


def partner(value, axis, apart):
    mask = 2**apart
    pairs = [(source, source ^ mask) for source in range(lax.axis_size(axis))]
    return lax.ppermute(value, axis, pairs)


def rope_tables(length, width, offset):
    half_width = width // 2
    positions = (offset + jnp.arange(length)).astype(jnp.float32)
    exponent = jnp.arange(half_width).astype(jnp.float32) * (2.0 / width)
    frequency = jnp.power(jnp.float32(ROPE_BASE), -exponent)
    angles = positions[:, None] * frequency[None, :]
    return (jnp.cos(angles), jnp.sin(angles))


def rotate(vectors, cosine, sine):
    half_width = vectors.shape[-1] // 2
    first = vectors[..., :half_width]
    second = vectors[..., half_width:]
    cosine = cosine[:, None, :]
    sine = sine[:, None, :]
    return jnp.concatenate(
        [first * cosine - second * sine, second * cosine + first * sine], axis=-1
    )


def feature_map(vectors, weights):
    logits = jnp.einsum("thd,hdf->thf", vectors, weights, precision=MATMUL_ACCURACY)
    upper = jnp.exp(logits)
    lower = jnp.exp(-logits)
    return jnp.concatenate(
        [upper / jnp.sum(upper, -1, keepdims=True), lower / jnp.sum(lower, -1, keepdims=True)],
        axis=-1,
    )


def teacher_kernel(first_ref, query_ref, key_ref, value_ref, out_ref):
    rows = query_ref.shape[0]
    block = rows // 2 if rows % 2 == 0 else rows
    first = first_ref[0]
    scale = 1.0 / math.sqrt(query_ref.shape[1])
    queries = query_ref[...]

    def scored(start):
        keys = key_ref[pl.ds(start, block), :]
        scores = lax.dot_general(
            queries, keys, (((1,), (1,)), ((), ())), preferred_element_type=jnp.float32
        )
        return scores * scale

    def add(carry, weights, start):
        numerator, denominator = carry
        values = value_ref[pl.ds(start, block), :]
        denominator = denominator + jnp.sum(weights, axis=1, keepdims=True)
        numerator = numerator + jnp.dot(
            weights.astype(jnp.bfloat16), values, preferred_element_type=jnp.float32
        )
        return numerator, denominator

    def earlier(index, carry):
        start = pl.multiple_of(index * block, block)
        return add(carry, jnp.exp(scored(start)), start)

    carry = (
        jnp.zeros((rows, out_ref.shape[1]), jnp.float32),
        jnp.zeros((rows, 1), jnp.float32),
    )
    carry = lax.fori_loop(0, first // block, earlier, carry)
    for part in range(rows // block):
        start = pl.multiple_of(first + part * block, block)
        row = lax.broadcasted_iota(jnp.int32, (rows, block), 0)
        column = lax.broadcasted_iota(jnp.int32, (rows, block), 1) + part * block
        weights = jnp.exp(jnp.where(column <= row, scored(start), -1e30))
        carry = add(carry, weights, start)
    numerator, denominator = carry
    out_ref[...] = (numerator / denominator).astype(out_ref.dtype)


def teacher_attention(first, queries_rot, keys_rot, values):
    rows, width = queries_rot.shape
    span = keys_rot.shape[0]
    return pl.pallas_call(
        teacher_kernel,
        out_shape=jax.ShapeDtypeStruct((rows, width), jnp.bfloat16),
        grid_spec=pltpu.PrefetchScalarGridSpec(
            num_scalar_prefetch=1,
            grid=(width // DH,),
            in_specs=[
                pl.BlockSpec((rows, DH), lambda head, first: (0, head)),
                pl.BlockSpec((span, DH), lambda head, first: (0, 0)),
                pl.BlockSpec((span, DH), lambda head, first: (0, 0)),
            ],
            out_specs=pl.BlockSpec((rows, DH), lambda head, first: (0, head)),
        ),
        compiler_params=pltpu.CompilerParams(vmem_limit_bytes=32 * 1024 * 1024),
        cost_estimate=pl.CostEstimate(
            flops=4 * rows * span * width,
            bytes_accessed=4 * rows * width + 4 * span * DH,
            transcendentals=rows * span * (width // DH),
        ),
    )(jnp.reshape(first, (1,)).astype(jnp.int32), queries_rot, keys_rot, values)


def from_lower(value, shift):
    size = lax.axis_size("seq")
    return lax.ppermute(value, "seq", [(i, i + shift) for i in range(size - shift)])


def from_higher(value, shift):
    size = lax.axis_size("seq")
    return lax.ppermute(value, "seq", [(i + shift, i) for i in range(size - shift)])


def sum_of_others(arrays, receive):
    totals = [jnp.zeros(array.shape, jnp.float32) for array in arrays]
    for shift in range(1, lax.axis_size("seq")):
        for slot, array in enumerate(arrays):
            totals[slot] = totals[slot] + receive(array, shift).astype(jnp.float32)
    return totals


def gather_seq(piece):
    size = lax.axis_size("seq")
    rows = piece.shape[0]
    me = lax.axis_index("seq")
    whole = jnp.zeros((size * rows,) + piece.shape[1:], piece.dtype)
    whole = lax.dynamic_update_slice_in_dim(whole, piece, me * rows, 0)
    for shift in range(1, size):
        source = (me - shift + size) % size
        got = lax.ppermute(piece, "seq", [(i, (i + shift) % size) for i in range(size)])
        whole = lax.dynamic_update_slice_in_dim(whole, got, source * rows, 0)
    return whole


def token_blocks(tokens):
    size = lax.axis_size("head")
    me = lax.axis_index("head")
    if size != 8:
        gathered = lax.all_gather(tokens, "head", axis=1, tiled=True)
        return [(jnp.int32(0), gathered)]
    ring = size // 2
    z, x = me // 2, me % 2

    def up(value):
        return lax.ppermute(value, "head", [(s, (s + 2) % size) for s in range(size)])

    def down(value):
        return lax.ppermute(value, "head", [(s, (s + size - 2) % size) for s in range(size)])

    def across(value):
        return lax.ppermute(value, "head", [(s, s ^ 1) for s in range(size)])

    def index(dz, dx):
        return ((z + dz) % ring) * 2 + (x + dx) % 2

    half = tokens.shape[0] // 2
    below = up(tokens)
    above = down(tokens)
    beside = across(tokens)
    far = jnp.concatenate([up(below[:half]), down(above[half:])], 0)
    beside_below = up(beside)
    beside_above = down(beside)
    beside_far = across(far)
    return [
        (index(0, 0), tokens),
        (index(0, 1), beside),
        (index(ring - 1, 0), below),
        (index(1, 0), above),
        (index(2, 0), far),
        (index(ring - 1, 1), beside_below),
        (index(1, 1), beside_above),
        (index(2, 1), beside_far),
    ]


def per_device_by_rows(tokens, w_query, w_key, w_value, map_query, map_key):
    row_count = tokens.shape[0]
    head_count = w_query.shape[1] // DH
    shared_width = w_key.shape[1]
    w_pair = jnp.concatenate([w_key, w_value], 1)
    query_rows = jnp.zeros((row_count, w_query.shape[1]), jnp.float32)
    pair_rows = jnp.zeros((row_count, w_pair.shape[1]), jnp.float32)
    for position, block in token_blocks(tokens):
        depth = block.shape[1]
        weights = lax.dynamic_slice_in_dim(w_query, position * depth, depth, 0)
        pair_weights = lax.dynamic_slice_in_dim(w_pair, position * depth, depth, 0)
        query_rows = query_rows + jnp.dot(block, weights, preferred_element_type=jnp.float32)
        pair_rows = pair_rows + jnp.dot(block, pair_weights, preferred_element_type=jnp.float32)
    keys = pair_rows[:, :shared_width]
    values = pair_rows[:, shared_width:]
    keys = keys.astype(jnp.bfloat16)
    values = values.astype(jnp.bfloat16)
    if shared_width < DH:
        partner_keys, partner_values = partner((keys, values), "head", 0)
        upper_half = lax.axis_index("head") % 2 == 1
        keys = jnp.where(
            upper_half,
            jnp.concatenate([partner_keys, keys], 1),
            jnp.concatenate([keys, partner_keys], 1),
        )
        values = jnp.where(
            upper_half,
            jnp.concatenate([partner_values, values], 1),
            jnp.concatenate([values, partner_values], 1),
        )
    chain_index = lax.axis_index("seq")
    query_first = chain_index * row_count
    cosine, sine = rope_tables(row_count, DH, query_first)
    queries_rot = rotate(query_rows.reshape(row_count, head_count, DH), cosine, sine).astype(
        jnp.bfloat16
    )
    keys_rot = (
        rotate(keys.astype(jnp.float32).reshape(row_count, 1, DH), cosine, sine)
        .reshape(row_count, DH)
        .astype(jnp.bfloat16)
    )
    pair_all = gather_seq(jnp.concatenate([keys_rot, values], 1))
    teacher = teacher_attention(
        query_first,
        queries_rot.reshape(row_count, head_count * DH),
        pair_all[:, :DH],
        pair_all[:, DH:],
    )
    query_float = queries_rot.astype(jnp.float32)
    key_float = jnp.broadcast_to(
        keys_rot.astype(jnp.float32)[:, None, :], (row_count, head_count, DH)
    )
    value_single_float = values.astype(jnp.float32)
    query_features = feature_map(query_float, map_query)
    key_features = feature_map(key_float, map_key)
    state_local = jnp.einsum(
        "thf,td->hfd", key_features, value_single_float, precision=MATMUL_ACCURACY
    )
    norm_local = jnp.sum(key_features, 0)
    state_before, norm_before = sum_of_others(
        (state_local.astype(jnp.bfloat16), norm_local), from_lower
    )
    local_mask = (jnp.arange(row_count)[None, :] <= jnp.arange(row_count)[:, None]).astype(
        jnp.float32
    )

    def student_local(query_feature_rows, key_feature_rows, state, norm):
        within = (
            jnp.einsum(
                "ueo,aeo->eua", query_feature_rows, key_feature_rows, precision=MATMUL_ACCURACY
            )
            * local_mask[None]
        )
        upper = jnp.einsum("hqk,kd->qhd", within, value_single_float, precision=MATMUL_ACCURACY)
        upper = upper + jnp.einsum(
            "qhf,hfd->qhd", query_feature_rows, state, precision=MATMUL_ACCURACY
        )
        lower = jnp.transpose(jnp.sum(within, -1)) + jnp.einsum(
            "qhf,hf->qh", query_feature_rows, norm, precision=MATMUL_ACCURACY
        )
        return upper / lower[..., None]

    student, pullback = jax.vjp(
        student_local, query_features, key_features, state_before, norm_before
    )
    student_out = student.astype(jnp.bfloat16).reshape(row_count, head_count * DH)
    target = teacher.reshape(row_count, head_count, DH).astype(jnp.float32)
    grad_student = 2.0 * (student - target)
    grad_query_feat, grad_key_feat, grad_state, grad_norm = pullback(grad_student)
    state_after, norm_after = sum_of_others(
        (grad_state.astype(jnp.bfloat16), grad_norm), from_higher
    )
    grad_key_feat = (
        grad_key_feat
        + jnp.einsum("td,hfd->thf", value_single_float, state_after, precision=MATMUL_ACCURACY)
        + norm_after[None]
    )
    unused_query, query_backward = jax.vjp(
        lambda weights: feature_map(query_float, weights), map_query
    )
    unused_key, pull_key = jax.vjp(lambda weights: feature_map(key_float, weights), map_key)
    grad_query = query_backward(grad_query_feat)[0]
    grad_key = pull_key(grad_key_feat)[0]
    features = grad_query.shape[-1]
    grads = jnp.concatenate([grad_query, grad_key], -1)
    size = lax.axis_size("seq")
    if size & (size - 1):
        grads = lax.psum(grads, "seq")
    else:
        apart = 0
        while 2**apart < size:
            if apart > 0:
                sent = grads.astype(jnp.bfloat16)
                grads = sent.astype(jnp.float32) + partner(sent, "seq", apart).astype(jnp.float32)
            else:
                grads = grads + partner(grads, "seq", apart)
            apart += 1
    grad_query, grad_key = grads[..., :features], grads[..., features:]
    return (student_out, grad_query, grad_key)


F32 = jnp.float32
BF16 = jnp.bfloat16
MESH = pl.DeviceIdType.MESH


def dot_nn(a, b):
    return lax.dot_general(a, b, (((1,), (0,)), ((), ())), preferred_element_type=F32)
def dot_nt(a, b):
    return lax.dot_general(a, b, (((1,), (1,)), ((), ())), preferred_element_type=F32)
def dot_tn(a, b):
    return lax.dot_general(a, b, (((0,), (0,)), ((), ())), preferred_element_type=F32)

def split(v):
    high = v.astype(BF16)
    low = (v - high.astype(F32)).astype(BF16)
    return high, low

def half_sums(v, ones):
    high, low = split(v)
    return dot_nn(jnp.concatenate([high, low], 1), ones)

def attention_kernel(C, q_hbm, kv_hbm, mapq_hbm, mapk_hbm, out_hbm, gradq_ref, gradk_ref,
                     q_ref, kv_ref, mq_ref, mk_ref, out_ref, vaug, tch, qf, kf, qfb, kfb, dk, gu, student, inverse, stb, state, gsum, mq, mk,
                     wq, wk, land, load_sem, piece_sem, out_send, out_recv, own_sem, grad_send, grad_recv):
    T = q_ref.shape[0]
    W = out_hbm.shape[0]
    size = lax.axis_size("seq")
    me = lax.axis_index("seq")
    barrier = pltpu.get_barrier_semaphore()
    for shift in range(1, size):
        pl.semaphore_signal(barrier, 1, device_id={"seq": lax.rem(me + shift, size)}, device_id_type=MESH)
    heads_here = pl.ds(me * (q_ref.shape[1] // DH), q_ref.shape[1] // DH)
    loads = [pltpu.make_async_copy(src, dst, load_sem.at[n]) for n, (src, dst) in enumerate((
        (mapq_hbm.at[heads_here], mq_ref), (mapk_hbm.at[heads_here], mk_ref)))]

    def pieces(n):
        at = pl.ds(pl.multiple_of(n * W, W), W)
        return [pltpu.make_async_copy(src.at[at], dst.at[at], piece_sem.at[m, n])
                for m, (src, dst) in enumerate(((kv_hbm, kv_ref), (q_hbm, q_ref)))]
    for copy in loads:
        copy.start()
    for n in range(size):
        for copy in pieces(n):
            copy.start()
    pl.semaphore_wait(barrier, size - 1)
    for copy in loads:
        copy.wait()
    H = q_ref.shape[1] // DH
    tiles = T // C
    scale = math.log2(math.e) / math.sqrt(DH)
    r = lax.broadcasted_iota(jnp.int32, (2 * DH, DH), 0)
    c = lax.broadcasted_iota(jnp.int32, (2 * DH, DH), 1)
    half = DH // 2
    ones = jnp.where((r % DH) // half == c // half, 1.0, 0.0).astype(BF16)
    row = lax.broadcasted_iota(jnp.int32, (C, C), 0)
    column = lax.broadcasted_iota(jnp.int32, (C, C), 1)
    causal = column <= row
    for h in range(H):
        for src, dst in ((mq_ref, wq), (mk_ref, wk)):
            w = src[h].T
            high, low = split(jnp.concatenate([w, -w], 1))
            dst[h] = jnp.concatenate([high, low], 0)
    state[...] = jnp.zeros_like(state)
    gsum[...] = jnp.zeros_like(gsum)
    mq[...] = jnp.zeros_like(mq)
    mk[...] = jnp.zeros_like(mk)

    def rows_of(i):
        return pl.ds(pl.multiple_of(i * C, C), C)

    def features(i, carry):
        @pl.when(lax.rem(i, W // C) == 0)
        def _():
            for copy in pieces(i // (W // C)):
                copy.wait()
        rows = rows_of(i)
        k = kv_ref[rows, :DH]
        vaug[rows, :DH] = kv_ref[rows, DH:]
        vaug[rows, DH:] = jnp.ones((C, DH), BF16)
        k2 = jnp.concatenate([k, k], 1)
        for h in range(H):
            cols = slice(h * DH, (h + 1) * DH)
            q = q_ref[rows, cols]
            for x2, w, f, fb in ((jnp.concatenate([q, q], 1), wq, qf, qfb), (k2, wk, kf, kfb)):
                e = jnp.exp(dot_nn(x2, w[h]))
                phi = e / half_sums(e, ones)
                f[rows, cols] = phi
                fb[rows, cols] = phi.astype(BF16)
        return carry
    lax.fori_loop(0, tiles, features, 0, unroll=2)

    def phi_back(phi, d):
        return (phi * (d - half_sums(d * phi, ones))).astype(BF16)

    big = W // C
    heads = range(H)
    width = H * DH

    def out_copy(i, local):
        owner = i // big
        to = out_hbm.at[pl.ds(pl.multiple_of(lax.rem(i, big) * C, C), C), pl.ds(pl.multiple_of(me * width, width), width)]
        if local:
            return pltpu.make_async_copy(out_ref.at[rows_of(i)], to, own_sem.at[lax.rem(i, big)])
        return pltpu.make_async_remote_copy(
            src_ref=out_ref.at[rows_of(i)], dst_ref=to, send_sem=out_send.at[i], recv_sem=out_recv.at[lax.rem(i, big), me],
            device_id={"seq": owner}, device_id_type=MESH)

    def give(i, act_local, act_remote):
        @pl.when(i // big == me)
        def _():
            act_local(out_copy(i, True))
        @pl.when(i // big != me)
        def _():
            act_remote(out_copy(i, False))

    start = lambda copy: copy.start()

    def grad_copy(kind, shift):
        return pltpu.make_async_remote_copy(
            src_ref=land.at[kind, me], dst_ref=land.at[kind, me], send_sem=grad_send.at[kind, shift],
            recv_sem=grad_recv.at[kind, shift], device_id={"seq": lax.rem(me + shift, size)}, device_id_type=MESH)

    def give_grads(kind, total):
        for h in heads:
            v = total[h]
            land[kind, me, h] = (v[:, :half] - v[:, half:]).T
        for shift in range(1, size):
            grad_copy(kind, shift).start()

    def forward(i, carry):
        @pl.when(i > 0)
        def _():
            give(i - 1, start, start)
        rows = rows_of(i)
        va = vaug[rows, :]
        cols = [slice(h * DH, (h + 1) * DH) for h in heads]
        fq = [qfb[rows, cols[h]] for h in heads]
        fk = [kfb[rows, cols[h]] for h in heads]
        a = [jnp.where(causal, dot_nt(fq[h], fk[h]), 0.0).astype(BF16) for h in heads]
        av = dot_nn(jnp.concatenate(a, 0), va)
        for h in heads:
            st = state[h]
            before = st.astype(BF16)
            stb[i, h] = before
            state[h] = st + dot_tn(fk[h], va)
            nd = av[h * C:(h + 1) * C] + dot_nn(fq[h], before)
            inv = 1.0 / nd[:, DH:]
            y = nd[:, :DH] * inv
            out_ref[rows, cols[h]] = y.astype(out_ref.dtype)
            student[rows, cols[h]] = y
            inverse[rows, cols[h]] = inv
        return carry
    lax.fori_loop(0, tiles, forward, 0, unroll=2)
    give(tiles - 1, start, start)

    def teach(n, carry):
        first = n * big
        rows = pl.ds(pl.multiple_of(n * W, W), W)
        q = jnp.concatenate([q_ref[rows, h * DH:(h + 1) * DH] for h in heads], 0)

        def earlier(j, acc):
            seen = pl.ds(pl.multiple_of(j * W, W), W)
            s = dot_nt(q, kv_ref[seen, :DH]) * scale
            return acc + dot_nn(jnp.exp2(s).astype(BF16), vaug[seen, :])
        acc = lax.fori_loop(0, n, earlier, jnp.zeros((H * W, 2 * DH), F32))
        parts = []
        for b in range(big):
            seen = pl.ds(pl.multiple_of(n * W + b * C, C), C)
            q = jnp.concatenate([q_ref[pl.ds(pl.multiple_of(n * W + b * C, C), W - b * C), h * DH:(h + 1) * DH] for h in heads], 0)
            s = dot_nt(q, kv_ref[seen, :DH]) * scale
            left = W - b * C
            s = jnp.concatenate([x for h in heads for x in
                                 [jnp.where(causal, s[h * left:h * left + C], -1e30), s[h * left + C:(h + 1) * left]]], 0) if left > C else jnp.concatenate([jnp.where(causal, s[h * C:(h + 1) * C], -1e30) for h in heads], 0)
            p = dot_nn(jnp.exp2(s).astype(BF16), vaug[seen, :])
            parts.append(p)
        for h in heads:
            for b in range(big):
                v = acc[h * W + b * C:h * W + (b + 1) * C]
                for b2 in range(b + 1):
                    left = W - b2 * C
                    lo = h * left + (b - b2) * C
                    v = v + parts[b2][lo:lo + C]
                tch[pl.ds(pl.multiple_of(n * W + b * C, C), C), h * DH:(h + 1) * DH] = (v[:, :DH] / v[:, DH:]).astype(BF16)
        return carry
    lax.fori_loop(0, T // W, teach, 0)

    def gradient(i, carry):
        rows = rows_of(i)
        va = vaug[rows, :]
        cols = [slice(h * DH, (h + 1) * DH) for h in heads]
        fq = [qfb[rows, cols[h]] for h in heads]
        fk = [kfb[rows, cols[h]] for h in heads]
        dua = []
        for h in heads:
            y = student[rows, cols[h]]
            du = ((2.0 * (y - tch[rows, cols[h]].astype(F32))) * inverse[rows, cols[h]]).astype(BF16)
            dl = jnp.sum(du.astype(F32) * y, 1, keepdims=True) * (-1.0 / half)
            dl_high, dl_low = split(dl)
            dua.append(jnp.concatenate([du, jnp.broadcast_to(dl_high, (C, half)), jnp.broadcast_to(dl_low, (C, half))], 1))
        dall = dot_nt(jnp.concatenate(dua, 0), va)
        for h in heads:
            da = jnp.where(causal, dall[h * C:(h + 1) * C], 0.0).astype(BF16)
            dq = dot_nn(da, fk[h]) + dot_nt(dua[h], stb[i, h])
            dk[rows, cols[h]] = dot_tn(da, fq[h])
            gu[i, h] = dot_tn(fq[h], dua[h])
            g = phi_back(qf[rows, cols[h]], dq)
            mq[h] += dot_tn(q_ref[rows, cols[h]], g)
        return carry
    lax.fori_loop(0, tiles, gradient, 0, unroll=2)
    give_grads(0, mq)

    def backward(n, carry):
        i = tiles - 1 - n
        rows = rows_of(i)
        va = vaug[rows, :]
        keys = kv_ref[rows, :DH]
        for h in range(H):
            cols = slice(h * DH, (h + 1) * DH)
            d = dk[rows, cols] + dot_nt(va, gsum[h].astype(BF16))
            g = phi_back(kf[rows, cols], d)
            mk[h] += dot_tn(keys, g)
            gsum[h] += gu[i, h]
        return carry
    lax.fori_loop(0, tiles, backward, 0, unroll=2)
    give_grads(1, mk)

    def finish(i, carry):
        give(i, lambda copy: copy.wait(), lambda copy: copy.wait_send())
        return carry
    lax.fori_loop(0, tiles, finish, 0)
    for b in range(big):
        for shift in range(1, size):
            source = lax.rem(me + shift, size)
            pltpu.make_async_remote_copy(
                src_ref=out_ref.at[rows_of(b)],
                dst_ref=out_hbm.at[pl.ds(b * C, C), pl.ds(pl.multiple_of(source * width, width), width)],
                send_sem=out_send.at[b], recv_sem=out_recv.at[b, source],
                device_id={"seq": source}, device_id_type=MESH).wait_recv()
    for kind, ref in ((0, gradq_ref), (1, gradk_ref)):
        for shift in range(1, size):
            grad_copy(kind, shift).wait()
        for n in range(size):
            for h in heads:
                ref[n * H + h] = land[kind, n, h]


def attention(q, kv, map_query, map_key, rows, C=256):
    T, width = q.shape
    H = width // DH
    count = map_query.shape[0]
    map_query, map_key = jnp.swapaxes(map_query, 1, 2), jnp.swapaxes(map_key, 1, 2)
    size = lax.axis_size("seq")
    V = lambda *s: pltpu.VMEM(s, F32)
    B = lambda *s: pltpu.VMEM(s, BF16)
    dma = pltpu.SemaphoreType.DMA
    vm = pl.BlockSpec(memory_space=pltpu.VMEM)
    anywhere = pl.BlockSpec(memory_space=pl.ANY)
    grads = jax.ShapeDtypeStruct(map_query.shape, F32)
    maps = (H,) + map_query.shape[1:]
    tiles = T // C
    out, grad_query, grad_key = pl.pallas_call(
        functools.partial(attention_kernel, C),
        out_shape=(jax.ShapeDtypeStruct((rows, count * DH), BF16), grads, grads),
        in_specs=[anywhere] * 4,
        out_specs=(anywhere, vm, vm),
        scratch_shapes=[B(T, width), B(T, 2 * DH), V(*maps), V(*maps), B(T, width),
                        B(T, 2 * DH), B(T, width), V(T, width), V(T, width), B(T, width), B(T, width), V(T, width),
                        V(tiles, H, DH, 2 * DH), V(T, width), V(T, width), B(tiles, H, DH, 2 * DH), V(H, DH, 2 * DH), V(H, DH, 2 * DH), V(H, DH, DH), V(H, DH, DH),
                        B(H, 2 * DH, DH), B(H, 2 * DH, DH), V(2, size, H, DH // 2, DH),
                        dma((2,)), dma((2, size)), dma((tiles,)), dma((rows // C, size)), dma((rows // C,)), dma((2, size)), dma((2, size))],
        compiler_params=pltpu.CompilerParams(collective_id=1, has_side_effects=True, vmem_limit_bytes=60 * 2**20),
        cost_estimate=pl.CostEstimate(flops=4 * T * T * width, bytes_accessed=8 * T * width, transcendentals=T * T * H),
    )(q, kv, map_query, map_key)
    return out, jnp.swapaxes(grad_query, 1, 2), jnp.swapaxes(grad_key, 1, 2)


def project_kernel(chunk, t_hbm, wq_hbm, wk_hbm, wv_hbm, frequency_ref, q_out, kv_out,
                   cos_ref, sin_ref, tok, wq, wp, acc, stq, stkv, ssem, rsem, wsem, tsem, qsend, qrecv, ksend, krecv, own_sem):
    size = lax.axis_size("seq")
    me = lax.axis_index("seq")
    place = lax.axis_index("head")
    z, x = place // 2, place % 2
    last = lax.axis_size("head") // 2 - 1
    rows, depth = t_hbm.shape
    width = wq_hbm.shape[1]
    share = width // size
    chunks = rows // chunk
    half = chunks // 2
    above = jnp.minimum(z + 1, last) * 2 + x
    below = jnp.maximum(z - 1, 0) * 2 + x
    beside = z * 2 + 1 - x
    twin = z + 1 - 2 * (z % 2)
    e1 = twin
    e2 = jnp.where(z < 2, 2, 1)
    e3 = jnp.where(z < 2, 3, 0)

    barrier = pltpu.get_barrier_semaphore()
    @pl.when(z < last)
    def _():
        pl.semaphore_signal(barrier, 1, device_id={"head": above}, device_id_type=MESH)
    @pl.when(z > 0)
    def _():
        pl.semaphore_signal(barrier, 1, device_id={"head": below}, device_id_type=MESH)
    pl.semaphore_signal(barrier, 1, device_id={"head": beside}, device_id_type=MESH)
    for shift in range(1, size):
        pl.semaphore_signal(barrier, 1, device_id={"seq": lax.rem(me + shift, size)}, device_id_type=MESH)

    def load(d):
        at = pl.ds(pl.multiple_of(d * depth, depth), depth)
        return (
            pltpu.make_async_copy(wq_hbm.at[at], wq.at[at], wsem.at[0, d]),
            pltpu.make_async_copy(wk_hbm.at[at], wp.at[at, pl.ds(0, DH)], wsem.at[1, d]),
            pltpu.make_async_copy(wv_hbm.at[at], wp.at[at, pl.ds(DH, DH)], wsem.at[2, d]),
        )
    mine = pltpu.make_async_copy(t_hbm, tok.at[place], tsem)
    mine.start()
    order = [place, e1 * 2 + x, z * 2 + 1 - x, e2 * 2 + x, e1 * 2 + 1 - x, e3 * 2 + x, e2 * 2 + 1 - x, e3 * 2 + 1 - x]
    for d in order:
        for copy in load(d):
            copy.start()
    pl.semaphore_wait(barrier, size + jnp.where(z > 0, 1, 0) + jnp.where(z < last, 1, 0))

    def span(c):
        return pl.ds(pl.multiple_of(c * chunk, chunk), chunk)

    def send(c, d, kind, to, own=False):
        return pltpu.make_async_remote_copy(
            src_ref=t_hbm.at[span(c)] if own else tok.at[d, span(c)],
            dst_ref=tok.at[d, span(c)],
            send_sem=ssem.at[c, kind],
            recv_sem=rsem.at[c, d],
            device_id={"head": to},
            device_id_type=MESH,
        )

    def arrived(c, d):
        send(c, d, 0, beside).wait_recv()

    def own_sends(c, act):
        @pl.when(z < last)
        def _():
            act(send(c, place, 0, above, True))
        @pl.when(z > 0)
        def _():
            act(send(c, place, 1, below, True))
        act(send(c, place, 2, beside, True))

    def relays(c, n, e, act):
        d = e * 2 + x
        @pl.when((e > z) & (z > 0))
        def _():
            act(send(c, d, 2 + n, below))
        @pl.when((e < z) & (z < last))
        def _():
            act(send(c, d, 2 + n, above))
        if n == 1:
            @pl.when(c < half)
            def _():
                act(send(c, d, 5 + n, beside))
        else:
            act(send(c, d, 5 + n, beside))

    def twin_sends(act):
        def one(c, carry):
            act(send(c, beside, 9, twin * 2 + x))
            return carry
        lax.fori_loop(half, chunks, one, 0)

    def outputs(c, act, local):
        at = pl.ds(pl.multiple_of(me * rows + c * chunk, chunk), chunk)
        for shift in range(1, size):
            to = lax.rem(me + shift, size)
            act(pltpu.make_async_remote_copy(
                src_ref=stkv.at[c], dst_ref=kv_out.at[at], send_sem=ksend.at[c, shift], recv_sem=krecv.at[c, shift],
                device_id={"seq": to}, device_id_type=MESH))
            act(pltpu.make_async_remote_copy(
                src_ref=stq.at[c, to], dst_ref=q_out.at[at], send_sem=qsend.at[c, shift], recv_sem=qrecv.at[c, shift],
                device_id={"seq": to}, device_id_type=MESH))
        local(pltpu.make_async_copy(stkv.at[c], kv_out.at[at], own_sem.at[c, 0]))
        local(pltpu.make_async_copy(stq.at[c, me], q_out.at[at], own_sem.at[c, 1]))

    start = lambda copy: copy.start()

    def weights_of(d):
        for copy in load(d):
            copy.wait()

    def multiply(row, count, d, first=False):
        at = pl.ds(pl.multiple_of(d * depth, depth), depth)
        to = pl.ds(row, count)
        block = tok[d, to, :]
        for p in range(size):
            cols = slice(p * share, (p + 1) * share)
            v = dot_nn(block, wq[at, cols])
            acc[to, cols] = v if first else acc[to, cols] + v
        v = dot_nn(block, wp[at, :])
        acc[to, width:] = v if first else acc[to, width:] + v

    def each(low, high, body):
        def one(c, carry):
            body(c)
            return carry
        lax.fori_loop(low, high, one, 0)

    each(0, chunks, lambda c: own_sends(c, start))

    def tables(c):
        row = lax.broadcasted_iota(jnp.int32, (chunk, DH), 0) + (me * rows + c * chunk)
        lane = lax.broadcasted_iota(jnp.int32, (chunk, DH), 1)
        angle = row.astype(F32) * frequency_ref[:1, :]
        sine = jnp.sin(angle)
        cos_ref[span(c), :] = jnp.cos(angle)
        sin_ref[span(c), :] = jnp.where(lane < DH // 2, -sine, sine)
    each(0, chunks, tables)
    mine.wait()
    weights_of(place)
    multiply(0, rows, place, True)
    o1, o2, o3 = e1 * 2 + x, e2 * 2 + x, e3 * 2 + x
    f1, f2, f3 = e1 * 2 + 1 - x, e2 * 2 + 1 - x, e3 * 2 + 1 - x

    def column(n, e, d):
        def body(c):
            arrived(c, d)
            relays(c, n, e, start)
        return body
    inner = (z > 0) & (z < last)
    outer = jnp.logical_not(inner)

    def nearest(c):
        column(1, e1, o1)(c)
        @pl.when(inner)
        def _():
            column(2, e2, o2)(c)
    each(0, chunks, nearest)
    weights_of(o1)
    multiply(0, rows, o1)
    each(0, chunks, lambda c: arrived(c, beside))
    @pl.when(outer)
    def _():
        twin_sends(start)
    weights_of(beside)
    multiply(0, rows, beside)
    @pl.when(outer)
    def _():
        each(0, chunks, column(2, e2, o2))
    weights_of(o2)
    multiply(0, rows, o2)
    @pl.when(inner)
    def _():
        each(0, chunks, column(3, e3, o3))
        twin_sends(start)
    each(0, half, lambda c: arrived(c, f1))
    weights_of(f1)
    multiply(0, half * chunk, f1)
    weights_of(o3)
    weights_of(f2)
    weights_of(f3)

    def step(k, carry):
        @pl.when(k < chunks)
        def _():
            @pl.when(outer)
            def _():
                column(3, e3, o3)(k)
            row = pl.multiple_of(k * chunk, chunk)
            multiply(row, chunk, o3)
            arrived(k, f2)
            multiply(row, chunk, f2)
        @pl.when(k >= half)
        def _():
            c = k - half
            row = pl.multiple_of(c * chunk, chunk)
            @pl.when(c >= half)
            def _():
                arrived(c, f1)
                multiply(row, chunk, f1)
            arrived(c, f3)
            multiply(row, chunk, f3)
            cosine = cos_ref[span(c), :]
            sine = sin_ref[span(c), :]
            rotate_rows = lambda v: (v * cosine + pltpu.roll(v, DH // 2, 1) * sine).astype(BF16)
            per = share // DH
            stkv[c, :, :DH] = rotate_rows(acc[span(c), width:width + DH].astype(BF16).astype(F32))
            stkv[c, :, DH:] = acc[span(c), width + DH:].astype(BF16)
            for p in range(size):
                for h in range(per):
                    at = (p * per + h) * DH
                    stq[c, p, :, h * DH:(h + 1) * DH] = rotate_rows(acc[span(c), at:at + DH])
            outputs(c, start, start)
        return carry
    lax.fori_loop(0, chunks + half, step, 0)

    done = lambda copy: copy.wait_send()
    def finish(c):
        own_sends(c, done)
        for n, e in ((1, e1), (2, e2), (3, e3)):
            relays(c, n, e, done)
        outputs(c, lambda copy: copy.wait(), lambda copy: copy.wait())
    each(0, chunks, finish)
    twin_sends(done)

def frequencies():
    exponent = np.arange(DH // 2, dtype=np.float64) * (2.0 / DH)
    table = np.power(ROPE_BASE, -exponent).astype(np.float32)
    return jnp.asarray(np.tile(np.concatenate([table, table])[None], (8, 1)))


def project_exchange(tokens, w_query, w_key, w_value, chunks=8):
    size = lax.axis_size("seq")
    rows, depth = tokens.shape
    full, width = w_query.shape
    share = width // size
    chunk = rows // chunks
    blocks = full // depth
    any_ = pl.BlockSpec(memory_space=pl.ANY)
    vm = pl.BlockSpec(memory_space=pltpu.VMEM)
    dma = pltpu.SemaphoreType.DMA
    return pl.pallas_call(
        functools.partial(project_kernel, chunk),
        out_shape=(jax.ShapeDtypeStruct((rows * size, share), BF16), jax.ShapeDtypeStruct((rows * size, 2 * DH), BF16)),
        in_specs=[any_] * 4 + [vm],
        out_specs=(any_, any_),
        scratch_shapes=[
            pltpu.VMEM((rows, DH), F32),
            pltpu.VMEM((rows, DH), F32),
            pltpu.VMEM((blocks, rows, depth), BF16),
            pltpu.VMEM((full, width), BF16),
            pltpu.VMEM((full, 2 * DH), BF16),
            pltpu.VMEM((rows, width + 2 * DH), F32),
            pltpu.VMEM((chunks, size, chunk, share), BF16),
            pltpu.VMEM((chunks, chunk, 2 * DH), BF16),
            dma((chunks, 10)), dma((chunks, blocks)), dma((3, blocks)), dma,
            dma((chunks, size)), dma((chunks, size)), dma((chunks, size)), dma((chunks, size)), dma((chunks, 2)),
        ],
        compiler_params=pltpu.CompilerParams(collective_id=0, has_side_effects=True, vmem_limit_bytes=62 * 2**20),
        cost_estimate=pl.CostEstimate(flops=2 * rows * full * (width + 2 * DH), bytes_accessed=full * width * 2, transcendentals=0),
    )(tokens, w_query, w_key, w_value, frequencies())


def per_device_by_heads(tokens, w_query, w_key, w_value, map_query, map_key):
    row_count = tokens.shape[0]
    queries, pair = project_exchange(tokens, w_query, w_key, w_value)
    return attention(queries, pair, map_query, map_key, row_count)


def fits(mesh, tokens, w_query, w_key):
    heads = w_query.shape[1] // mesh.shape["head"] // DH
    rows = tokens.shape[0] // mesh.shape["seq"]
    return (
        mesh.shape["head"] == 8
        and w_key.shape[1] // mesh.shape["head"] == DH
        and heads % mesh.shape["seq"] == 0
        and rows % 256 == 0
    )


def solution(mesh):
    in_specs = (
        P("seq", "head"),
        P(None, "head"),
        P(None, "head"),
        P(None, "head"),
        P("head", None, None),
        P("head", None, None),
    )
    out_specs = (P("seq", "head"), P("head", None, None), P("head", None, None))

    def run(tokens, w_query, w_key, w_value, map_query, map_key):
        body = per_device_by_heads if fits(mesh, tokens, w_query, w_key) else per_device_by_rows
        return jax.shard_map(
            body, mesh=mesh, in_specs=in_specs, out_specs=out_specs, check_vma=False
        )(tokens, w_query, w_key, w_value, map_query, map_key)

    return run
```

```python
import functools
import math

import jax
import jax.numpy as jnp
import numpy as np
from jax import lax
from jax.experimental import pallas as pl
from jax.experimental.pallas import tpu as pltpu
from jax.sharding import PartitionSpec as P

DH = 128


ROPE_BASE = 500000.0
MATMUL_ACCURACY = lax.Precision.DEFAULT


def partner(value, axis, apart):
    mask = 2**apart
    pairs = [(source, source ^ mask) for source in range(lax.axis_size(axis))]
    return lax.ppermute(value, axis, pairs)


def rope_tables(length, width, offset):
    half_width = width // 2
    positions = (offset + jnp.arange(length)).astype(jnp.float32)
    exponent = jnp.arange(half_width).astype(jnp.float32) * (2.0 / width)
    frequency = jnp.power(jnp.float32(ROPE_BASE), -exponent)
    angles = positions[:, None] * frequency[None, :]
    return (jnp.cos(angles), jnp.sin(angles))


def rotate(vectors, cosine, sine):
    half_width = vectors.shape[-1] // 2
    first = vectors[..., :half_width]
    second = vectors[..., half_width:]
    cosine = cosine[:, None, :]
    sine = sine[:, None, :]
    return jnp.concatenate(
        [first * cosine - second * sine, second * cosine + first * sine], axis=-1
    )


def feature_map(vectors, weights):
    logits = jnp.einsum("thd,hdf->thf", vectors, weights, precision=MATMUL_ACCURACY)
    upper = jnp.exp(logits)
    lower = jnp.exp(-logits)
    return jnp.concatenate(
        [upper / jnp.sum(upper, -1, keepdims=True), lower / jnp.sum(lower, -1, keepdims=True)],
        axis=-1,
    )


def teacher_kernel(first_ref, query_ref, key_ref, value_ref, out_ref):
    rows = query_ref.shape[0]
    block = rows // 2 if rows % 2 == 0 else rows
    first = first_ref[0]
    scale = 1.0 / math.sqrt(query_ref.shape[1])
    queries = query_ref[...]

    def scored(start):
        keys = key_ref[pl.ds(start, block), :]
        scores = lax.dot_general(
            queries, keys, (((1,), (1,)), ((), ())), preferred_element_type=jnp.float32
        )
        return scores * scale

    def add(carry, weights, start):
        numerator, denominator = carry
        values = value_ref[pl.ds(start, block), :]
        denominator = denominator + jnp.sum(weights, axis=1, keepdims=True)
        numerator = numerator + jnp.dot(
            weights.astype(jnp.bfloat16), values, preferred_element_type=jnp.float32
        )
        return numerator, denominator

    def earlier(index, carry):
        start = pl.multiple_of(index * block, block)
        return add(carry, jnp.exp(scored(start)), start)

    carry = (
        jnp.zeros((rows, out_ref.shape[1]), jnp.float32),
        jnp.zeros((rows, 1), jnp.float32),
    )
    carry = lax.fori_loop(0, first // block, earlier, carry)
    for part in range(rows // block):
        start = pl.multiple_of(first + part * block, block)
        row = lax.broadcasted_iota(jnp.int32, (rows, block), 0)
        column = lax.broadcasted_iota(jnp.int32, (rows, block), 1) + part * block
        weights = jnp.exp(jnp.where(column <= row, scored(start), -1e30))
        carry = add(carry, weights, start)
    numerator, denominator = carry
    out_ref[...] = (numerator / denominator).astype(out_ref.dtype)


def teacher_attention(first, queries_rot, keys_rot, values):
    rows, width = queries_rot.shape
    span = keys_rot.shape[0]
    return pl.pallas_call(
        teacher_kernel,
        out_shape=jax.ShapeDtypeStruct((rows, width), jnp.bfloat16),
        grid_spec=pltpu.PrefetchScalarGridSpec(
            num_scalar_prefetch=1,
            grid=(width // DH,),
            in_specs=[
                pl.BlockSpec((rows, DH), lambda head, first: (0, head)),
                pl.BlockSpec((span, DH), lambda head, first: (0, 0)),
                pl.BlockSpec((span, DH), lambda head, first: (0, 0)),
            ],
            out_specs=pl.BlockSpec((rows, DH), lambda head, first: (0, head)),
        ),
        compiler_params=pltpu.CompilerParams(vmem_limit_bytes=32 * 1024 * 1024),
        cost_estimate=pl.CostEstimate(
            flops=4 * rows * span * width,
            bytes_accessed=4 * rows * width + 4 * span * DH,
            transcendentals=rows * span * (width // DH),
        ),
    )(jnp.reshape(first, (1,)).astype(jnp.int32), queries_rot, keys_rot, values)


def from_lower(value, shift):
    size = lax.axis_size("seq")
    return lax.ppermute(value, "seq", [(i, i + shift) for i in range(size - shift)])


def from_higher(value, shift):
    size = lax.axis_size("seq")
    return lax.ppermute(value, "seq", [(i + shift, i) for i in range(size - shift)])


def sum_of_others(arrays, receive):
    totals = [jnp.zeros(array.shape, jnp.float32) for array in arrays]
    for shift in range(1, lax.axis_size("seq")):
        for slot, array in enumerate(arrays):
            totals[slot] = totals[slot] + receive(array, shift).astype(jnp.float32)
    return totals


def gather_seq(piece):
    size = lax.axis_size("seq")
    rows = piece.shape[0]
    me = lax.axis_index("seq")
    whole = jnp.zeros((size * rows,) + piece.shape[1:], piece.dtype)
    whole = lax.dynamic_update_slice_in_dim(whole, piece, me * rows, 0)
    for shift in range(1, size):
        source = (me - shift + size) % size
        got = lax.ppermute(piece, "seq", [(i, (i + shift) % size) for i in range(size)])
        whole = lax.dynamic_update_slice_in_dim(whole, got, source * rows, 0)
    return whole


def token_blocks(tokens):
    size = lax.axis_size("head")
    me = lax.axis_index("head")
    if size != 8:
        gathered = lax.all_gather(tokens, "head", axis=1, tiled=True)
        return [(jnp.int32(0), gathered)]
    ring = size // 2
    z, x = me // 2, me % 2

    def up(value):
        return lax.ppermute(value, "head", [(s, (s + 2) % size) for s in range(size)])

    def down(value):
        return lax.ppermute(value, "head", [(s, (s + size - 2) % size) for s in range(size)])

    def across(value):
        return lax.ppermute(value, "head", [(s, s ^ 1) for s in range(size)])

    def index(dz, dx):
        return ((z + dz) % ring) * 2 + (x + dx) % 2

    half = tokens.shape[0] // 2
    below = up(tokens)
    above = down(tokens)
    beside = across(tokens)
    far = jnp.concatenate([up(below[:half]), down(above[half:])], 0)
    beside_below = up(beside)
    beside_above = down(beside)
    beside_far = across(far)
    return [
        (index(0, 0), tokens),
        (index(0, 1), beside),
        (index(ring - 1, 0), below),
        (index(1, 0), above),
        (index(2, 0), far),
        (index(ring - 1, 1), beside_below),
        (index(1, 1), beside_above),
        (index(2, 1), beside_far),
    ]


def per_device_by_rows(tokens, w_query, w_key, w_value, map_query, map_key):
    row_count = tokens.shape[0]
    head_count = w_query.shape[1] // DH
    shared_width = w_key.shape[1]
    w_pair = jnp.concatenate([w_key, w_value], 1)
    query_rows = jnp.zeros((row_count, w_query.shape[1]), jnp.float32)
    pair_rows = jnp.zeros((row_count, w_pair.shape[1]), jnp.float32)
    for position, block in token_blocks(tokens):
        depth = block.shape[1]
        weights = lax.dynamic_slice_in_dim(w_query, position * depth, depth, 0)
        pair_weights = lax.dynamic_slice_in_dim(w_pair, position * depth, depth, 0)
        query_rows = query_rows + jnp.dot(block, weights, preferred_element_type=jnp.float32)
        pair_rows = pair_rows + jnp.dot(block, pair_weights, preferred_element_type=jnp.float32)
    keys = pair_rows[:, :shared_width]
    values = pair_rows[:, shared_width:]
    keys = keys.astype(jnp.bfloat16)
    values = values.astype(jnp.bfloat16)
    if shared_width < DH:
        partner_keys, partner_values = partner((keys, values), "head", 0)
        upper_half = lax.axis_index("head") % 2 == 1
        keys = jnp.where(
            upper_half,
            jnp.concatenate([partner_keys, keys], 1),
            jnp.concatenate([keys, partner_keys], 1),
        )
        values = jnp.where(
            upper_half,
            jnp.concatenate([partner_values, values], 1),
            jnp.concatenate([values, partner_values], 1),
        )
    chain_index = lax.axis_index("seq")
    query_first = chain_index * row_count
    cosine, sine = rope_tables(row_count, DH, query_first)
    queries_rot = rotate(query_rows.reshape(row_count, head_count, DH), cosine, sine).astype(
        jnp.bfloat16
    )
    keys_rot = (
        rotate(keys.astype(jnp.float32).reshape(row_count, 1, DH), cosine, sine)
        .reshape(row_count, DH)
        .astype(jnp.bfloat16)
    )
    pair_all = gather_seq(jnp.concatenate([keys_rot, values], 1))
    teacher = teacher_attention(
        query_first,
        queries_rot.reshape(row_count, head_count * DH),
        pair_all[:, :DH],
        pair_all[:, DH:],
    )
    query_float = queries_rot.astype(jnp.float32)
    key_float = jnp.broadcast_to(
        keys_rot.astype(jnp.float32)[:, None, :], (row_count, head_count, DH)
    )
    value_single_float = values.astype(jnp.float32)
    query_features = feature_map(query_float, map_query)
    key_features = feature_map(key_float, map_key)
    state_local = jnp.einsum(
        "thf,td->hfd", key_features, value_single_float, precision=MATMUL_ACCURACY
    )
    norm_local = jnp.sum(key_features, 0)
    state_before, norm_before = sum_of_others(
        (state_local.astype(jnp.bfloat16), norm_local), from_lower
    )
    local_mask = (jnp.arange(row_count)[None, :] <= jnp.arange(row_count)[:, None]).astype(
        jnp.float32
    )

    def student_local(query_feature_rows, key_feature_rows, state, norm):
        within = (
            jnp.einsum(
                "ueo,aeo->eua", query_feature_rows, key_feature_rows, precision=MATMUL_ACCURACY
            )
            * local_mask[None]
        )
        upper = jnp.einsum("hqk,kd->qhd", within, value_single_float, precision=MATMUL_ACCURACY)
        upper = upper + jnp.einsum(
            "qhf,hfd->qhd", query_feature_rows, state, precision=MATMUL_ACCURACY
        )
        lower = jnp.transpose(jnp.sum(within, -1)) + jnp.einsum(
            "qhf,hf->qh", query_feature_rows, norm, precision=MATMUL_ACCURACY
        )
        return upper / lower[..., None]

    student, pullback = jax.vjp(
        student_local, query_features, key_features, state_before, norm_before
    )
    student_out = student.astype(jnp.bfloat16).reshape(row_count, head_count * DH)
    target = teacher.reshape(row_count, head_count, DH).astype(jnp.float32)
    grad_student = 2.0 * (student - target)
    grad_query_feat, grad_key_feat, grad_state, grad_norm = pullback(grad_student)
    state_after, norm_after = sum_of_others(
        (grad_state.astype(jnp.bfloat16), grad_norm), from_higher
    )
    grad_key_feat = (
        grad_key_feat
        + jnp.einsum("td,hfd->thf", value_single_float, state_after, precision=MATMUL_ACCURACY)
        + norm_after[None]
    )
    unused_query, query_backward = jax.vjp(
        lambda weights: feature_map(query_float, weights), map_query
    )
    unused_key, pull_key = jax.vjp(lambda weights: feature_map(key_float, weights), map_key)
    grad_query = query_backward(grad_query_feat)[0]
    grad_key = pull_key(grad_key_feat)[0]
    features = grad_query.shape[-1]
    grads = jnp.concatenate([grad_query, grad_key], -1)
    size = lax.axis_size("seq")
    if size & (size - 1):
        grads = lax.psum(grads, "seq")
    else:
        apart = 0
        while 2**apart < size:
            if apart > 0:
                sent = grads.astype(jnp.bfloat16)
                grads = sent.astype(jnp.float32) + partner(sent, "seq", apart).astype(jnp.float32)
            else:
                grads = grads + partner(grads, "seq", apart)
            apart += 1
    grad_query, grad_key = grads[..., :features], grads[..., features:]
    return (student_out, grad_query, grad_key)


F32 = jnp.float32
BF16 = jnp.bfloat16
MESH = pl.DeviceIdType.MESH


def dot_nn(a, b):
    return lax.dot_general(a, b, (((1,), (0,)), ((), ())), preferred_element_type=F32)
def dot_nt(a, b):
    return lax.dot_general(a, b, (((1,), (1,)), ((), ())), preferred_element_type=F32)
def dot_tn(a, b):
    return lax.dot_general(a, b, (((0,), (0,)), ((), ())), preferred_element_type=F32)

def split(v):
    high = v.astype(BF16)
    low = (v - high.astype(F32)).astype(BF16)
    return high, low

def half_sums(v, ones):
    high, low = split(v)
    return dot_nn(jnp.concatenate([high, low], 1), ones)

def attention_kernel(C, q_hbm, kv_hbm, mapq_hbm, mapk_hbm, out_hbm, gradq_ref, gradk_ref,
                     q_ref, kv_ref, mq_ref, mk_ref, out_ref, vaug, tch, qf, kf, qfb, kfb, dk, gu, student, inverse, stb, state, gsum, mq, mk,
                     wq, wk, land, load_sem, piece_sem, out_send, out_recv, own_sem, grad_send, grad_recv):
    T = q_ref.shape[0]
    W = out_hbm.shape[0]
    size = lax.axis_size("seq")
    me = lax.axis_index("seq")
    barrier = pltpu.get_barrier_semaphore()
    for shift in range(1, size):
        pl.semaphore_signal(barrier, 1, device_id={"seq": lax.rem(me + shift, size)}, device_id_type=MESH)
    heads_here = pl.ds(me * (q_ref.shape[1] // DH), q_ref.shape[1] // DH)
    loads = [pltpu.make_async_copy(src, dst, load_sem.at[n]) for n, (src, dst) in enumerate((
        (mapq_hbm.at[heads_here], mq_ref), (mapk_hbm.at[heads_here], mk_ref)))]

    def pieces(n):
        at = pl.ds(pl.multiple_of(n * W, W), W)
        return [pltpu.make_async_copy(src.at[at], dst.at[at], piece_sem.at[m, n])
                for m, (src, dst) in enumerate(((kv_hbm, kv_ref), (q_hbm, q_ref)))]
    for copy in loads:
        copy.start()
    for n in range(size):
        for copy in pieces(n):
            copy.start()
    pl.semaphore_wait(barrier, size - 1)
    for copy in loads:
        copy.wait()
    H = q_ref.shape[1] // DH
    tiles = T // C

    def trips(most):
        return next(n for n in range(most, 0, -1) if tiles % n == 0)

    scale = math.log2(math.e) / math.sqrt(DH)
    r = lax.broadcasted_iota(jnp.int32, (2 * DH, DH), 0)
    c = lax.broadcasted_iota(jnp.int32, (2 * DH, DH), 1)
    half = DH // 2
    ones = jnp.where((r % DH) // half == c // half, 1.0, 0.0).astype(BF16)
    row = lax.broadcasted_iota(jnp.int32, (C, C), 0)
    column = lax.broadcasted_iota(jnp.int32, (C, C), 1)
    causal = column <= row
    for h in range(H):
        for src, dst in ((mq_ref, wq), (mk_ref, wk)):
            w = src[h].T
            high, low = split(jnp.concatenate([w, -w], 1))
            dst[h] = jnp.concatenate([high, low], 0)
    state[...] = jnp.zeros_like(state)
    gsum[...] = jnp.zeros_like(gsum)
    mq[...] = jnp.zeros_like(mq)
    mk[...] = jnp.zeros_like(mk)

    def rows_of(i):
        return pl.ds(pl.multiple_of(i * C, C), C)

    def features(i, carry):
        @pl.when(lax.rem(i, W // C) == 0)
        def _():
            for copy in pieces(i // (W // C)):
                copy.wait()
        rows = rows_of(i)
        k = kv_ref[rows, :DH]
        vaug[rows, :DH] = kv_ref[rows, DH:]
        vaug[rows, DH:] = jnp.ones((C, DH), BF16)
        k2 = jnp.concatenate([k, k], 1)
        for h in range(H):
            cols = slice(h * DH, (h + 1) * DH)
            q = q_ref[rows, cols]
            for x2, w, f, fb in ((jnp.concatenate([q, q], 1), wq, qf, qfb), (k2, wk, kf, kfb)):
                e = jnp.exp(dot_nn(x2, w[h]))
                phi = e / half_sums(e, ones)
                f[rows, cols] = phi
                fb[rows, cols] = phi.astype(BF16)
        return carry
    lax.fori_loop(0, tiles, features, 0, unroll=trips(4))

    def phi_back(phi, d):
        return (phi * (d - half_sums(d * phi, ones))).astype(BF16)

    big = W // C
    heads = range(H)
    width = H * DH

    def out_copy(i, local):
        owner = i // big
        to = out_hbm.at[pl.ds(pl.multiple_of(lax.rem(i, big) * C, C), C), pl.ds(pl.multiple_of(me * width, width), width)]
        if local:
            return pltpu.make_async_copy(out_ref.at[rows_of(i)], to, own_sem.at[lax.rem(i, big)])
        return pltpu.make_async_remote_copy(
            src_ref=out_ref.at[rows_of(i)], dst_ref=to, send_sem=out_send.at[i], recv_sem=out_recv.at[lax.rem(i, big), me],
            device_id={"seq": owner}, device_id_type=MESH)

    def give(i, act_local, act_remote):
        @pl.when(i // big == me)
        def _():
            act_local(out_copy(i, True))
        @pl.when(i // big != me)
        def _():
            act_remote(out_copy(i, False))

    start = lambda copy: copy.start()

    def grad_copy(kind, shift):
        return pltpu.make_async_remote_copy(
            src_ref=land.at[kind, me], dst_ref=land.at[kind, me], send_sem=grad_send.at[kind, shift],
            recv_sem=grad_recv.at[kind, shift], device_id={"seq": lax.rem(me + shift, size)}, device_id_type=MESH)

    def give_grads(kind, total):
        for h in heads:
            v = total[h]
            land[kind, me, h] = (v[:, :half] - v[:, half:]).T
        for shift in range(1, size):
            grad_copy(kind, shift).start()

    def forward(i, carry):
        @pl.when(i > 0)
        def _():
            give(i - 1, start, start)
        rows = rows_of(i)
        va = vaug[rows, :]
        cols = [slice(h * DH, (h + 1) * DH) for h in heads]
        fq = [qfb[rows, cols[h]] for h in heads]
        fk = [kfb[rows, cols[h]] for h in heads]
        a = [jnp.where(causal, dot_nt(fq[h], fk[h]), 0.0).astype(BF16) for h in heads]
        av = dot_nn(jnp.concatenate(a, 0), va)
        for h in heads:
            st = state[h]
            before = st.astype(BF16)
            stb[i, h] = before
            state[h] = st + dot_tn(fk[h], va)
            nd = av[h * C:(h + 1) * C] + dot_nn(fq[h], before)
            inv = 1.0 / nd[:, DH:]
            y = nd[:, :DH] * inv
            out_ref[rows, cols[h]] = y.astype(out_ref.dtype)
            student[rows, cols[h]] = y
            inverse[rows, cols[h]] = inv
        return carry
    lax.fori_loop(0, tiles, forward, 0, unroll=trips(3))
    give(tiles - 1, start, start)

    def teach(n, carry):
        first = n * big
        rows = pl.ds(pl.multiple_of(n * W, W), W)
        q = jnp.concatenate([q_ref[rows, h * DH:(h + 1) * DH] for h in heads], 0)

        def earlier(j, acc):
            seen = pl.ds(pl.multiple_of(j * W, W), W)
            s = dot_nt(q, kv_ref[seen, :DH]) * scale
            return acc + dot_nn(jnp.exp2(s).astype(BF16), vaug[seen, :])
        acc = lax.fori_loop(0, n, earlier, jnp.zeros((H * W, 2 * DH), F32))
        parts = []
        for b in range(big):
            seen = pl.ds(pl.multiple_of(n * W + b * C, C), C)
            q = jnp.concatenate([q_ref[pl.ds(pl.multiple_of(n * W + b * C, C), W - b * C), h * DH:(h + 1) * DH] for h in heads], 0)
            s = dot_nt(q, kv_ref[seen, :DH]) * scale
            left = W - b * C
            s = jnp.concatenate([x for h in heads for x in
                                 [jnp.where(causal, s[h * left:h * left + C], -1e30), s[h * left + C:(h + 1) * left]]], 0) if left > C else jnp.concatenate([jnp.where(causal, s[h * C:(h + 1) * C], -1e30) for h in heads], 0)
            p = dot_nn(jnp.exp2(s).astype(BF16), vaug[seen, :])
            parts.append(p)
        for h in heads:
            for b in range(big):
                v = acc[h * W + b * C:h * W + (b + 1) * C]
                for b2 in range(b + 1):
                    left = W - b2 * C
                    lo = h * left + (b - b2) * C
                    v = v + parts[b2][lo:lo + C]
                tch[pl.ds(pl.multiple_of(n * W + b * C, C), C), h * DH:(h + 1) * DH] = (v[:, :DH] / v[:, DH:]).astype(BF16)
        return carry
    lax.fori_loop(0, T // W, teach, 0, unroll=True)

    def gradient(i, carry):
        rows = rows_of(i)
        va = vaug[rows, :]
        cols = [slice(h * DH, (h + 1) * DH) for h in heads]
        fq = [qfb[rows, cols[h]] for h in heads]
        fk = [kfb[rows, cols[h]] for h in heads]
        dua = []
        for h in heads:
            y = student[rows, cols[h]]
            du = ((2.0 * (y - tch[rows, cols[h]].astype(F32))) * inverse[rows, cols[h]]).astype(BF16)
            dl = jnp.sum(du.astype(F32) * y, 1, keepdims=True) * (-1.0 / half)
            dl_high, dl_low = split(dl)
            dua.append(jnp.concatenate([du, jnp.broadcast_to(dl_high, (C, half)), jnp.broadcast_to(dl_low, (C, half))], 1))
        dall = dot_nt(jnp.concatenate(dua, 0), va)
        for h in heads:
            da = jnp.where(causal, dall[h * C:(h + 1) * C], 0.0).astype(BF16)
            dq = dot_nn(da, fk[h]) + dot_nt(dua[h], stb[i, h])
            dk[rows, cols[h]] = dot_tn(da, fq[h])
            gu[i, h] = dot_tn(fq[h], dua[h])
            g = phi_back(qf[rows, cols[h]], dq)
            mq[h] += dot_tn(q_ref[rows, cols[h]], g)
        return carry
    lax.fori_loop(0, tiles, gradient, 0, unroll=trips(3))
    give_grads(0, mq)

    def backward(n, carry):
        i = tiles - 1 - n
        rows = rows_of(i)
        va = vaug[rows, :]
        keys = kv_ref[rows, :DH]
        for h in range(H):
            cols = slice(h * DH, (h + 1) * DH)
            d = dk[rows, cols] + dot_nt(va, gsum[h].astype(BF16))
            g = phi_back(kf[rows, cols], d)
            mk[h] += dot_tn(keys, g)
            gsum[h] += gu[i, h]
        return carry
    lax.fori_loop(0, tiles, backward, 0, unroll=trips(4))
    give_grads(1, mk)

    def finish(i, carry):
        give(i, lambda copy: copy.wait(), lambda copy: copy.wait_send())
        return carry
    lax.fori_loop(0, tiles, finish, 0)
    for b in range(big):
        for shift in range(1, size):
            source = lax.rem(me + shift, size)
            pltpu.make_async_remote_copy(
                src_ref=out_ref.at[rows_of(b)],
                dst_ref=out_hbm.at[pl.ds(b * C, C), pl.ds(pl.multiple_of(source * width, width), width)],
                send_sem=out_send.at[b], recv_sem=out_recv.at[b, source],
                device_id={"seq": source}, device_id_type=MESH).wait_recv()
    for kind, ref in ((0, gradq_ref), (1, gradk_ref)):
        for shift in range(1, size):
            grad_copy(kind, shift).wait()
        for n in range(size):
            for h in heads:
                ref[n * H + h] = land[kind, n, h]


def attention(q, kv, map_query, map_key, rows, C=256):
    T, width = q.shape
    H = width // DH
    count = map_query.shape[0]
    map_query, map_key = jnp.swapaxes(map_query, 1, 2), jnp.swapaxes(map_key, 1, 2)
    size = lax.axis_size("seq")
    V = lambda *s: pltpu.VMEM(s, F32)
    B = lambda *s: pltpu.VMEM(s, BF16)
    dma = pltpu.SemaphoreType.DMA
    vm = pl.BlockSpec(memory_space=pltpu.VMEM)
    anywhere = pl.BlockSpec(memory_space=pl.ANY)
    grads = jax.ShapeDtypeStruct(map_query.shape, F32)
    maps = (H,) + map_query.shape[1:]
    tiles = T // C
    out, grad_query, grad_key = pl.pallas_call(
        functools.partial(attention_kernel, C),
        out_shape=(jax.ShapeDtypeStruct((rows, count * DH), BF16), grads, grads),
        in_specs=[anywhere] * 4,
        out_specs=(anywhere, vm, vm),
        scratch_shapes=[B(T, width), B(T, 2 * DH), V(*maps), V(*maps), B(T, width),
                        B(T, 2 * DH), B(T, width), V(T, width), V(T, width), B(T, width), B(T, width), V(T, width),
                        V(tiles, H, DH, 2 * DH), V(T, width), V(T, width), B(tiles, H, DH, 2 * DH), V(H, DH, 2 * DH), V(H, DH, 2 * DH), V(H, DH, DH), V(H, DH, DH),
                        B(H, 2 * DH, DH), B(H, 2 * DH, DH), V(2, size, H, DH // 2, DH),
                        dma((2,)), dma((2, size)), dma((tiles,)), dma((rows // C, size)), dma((rows // C,)), dma((2, size)), dma((2, size))],
        compiler_params=pltpu.CompilerParams(collective_id=1, has_side_effects=True, vmem_limit_bytes=46 * 2**20),
        cost_estimate=pl.CostEstimate(flops=4 * T * T * width, bytes_accessed=8 * T * width, transcendentals=T * T * H),
    )(q, kv, map_query, map_key)
    return out, jnp.swapaxes(grad_query, 1, 2), jnp.swapaxes(grad_key, 1, 2)


def project_kernel(chunk, t_hbm, wq_hbm, wk_hbm, wv_hbm, frequency_ref, q_out, kv_out,
                   cos_ref, sin_ref, tok, wq, wp, acc, stq, stkv, ssem, rsem, wsem, tsem, qsend, qrecv, ksend, krecv, own_sem):
    size = lax.axis_size("seq")
    me = lax.axis_index("seq")
    place = lax.axis_index("head")
    z, x = place // 2, place % 2
    last = lax.axis_size("head") // 2 - 1
    rows, depth = t_hbm.shape
    width = wq_hbm.shape[1]
    share = width // size
    chunks = rows // chunk
    half = chunks // 2
    above = jnp.minimum(z + 1, last) * 2 + x
    below = jnp.maximum(z - 1, 0) * 2 + x
    beside = z * 2 + 1 - x
    twin = z + 1 - 2 * (z % 2)
    e1 = twin
    e2 = jnp.where(z < 2, 2, 1)
    e3 = jnp.where(z < 2, 3, 0)

    barrier = pltpu.get_barrier_semaphore()
    @pl.when(z < last)
    def _():
        pl.semaphore_signal(barrier, 1, device_id={"head": above}, device_id_type=MESH)
    @pl.when(z > 0)
    def _():
        pl.semaphore_signal(barrier, 1, device_id={"head": below}, device_id_type=MESH)
    pl.semaphore_signal(barrier, 1, device_id={"head": beside}, device_id_type=MESH)
    for shift in range(1, size):
        pl.semaphore_signal(barrier, 1, device_id={"seq": lax.rem(me + shift, size)}, device_id_type=MESH)

    def load(d):
        at = pl.ds(pl.multiple_of(d * depth, depth), depth)
        return (
            pltpu.make_async_copy(wq_hbm.at[at], wq.at[at], wsem.at[0, d]),
            pltpu.make_async_copy(wk_hbm.at[at], wp.at[at, pl.ds(0, DH)], wsem.at[1, d]),
            pltpu.make_async_copy(wv_hbm.at[at], wp.at[at, pl.ds(DH, DH)], wsem.at[2, d]),
        )
    mine = pltpu.make_async_copy(t_hbm, tok.at[place], tsem)
    mine.start()
    order = [place, e1 * 2 + x, z * 2 + 1 - x, e2 * 2 + x, e1 * 2 + 1 - x, e3 * 2 + x, e2 * 2 + 1 - x, e3 * 2 + 1 - x]
    for d in order:
        for copy in load(d):
            copy.start()
    pl.semaphore_wait(barrier, size + jnp.where(z > 0, 1, 0) + jnp.where(z < last, 1, 0))

    def span(c):
        return pl.ds(pl.multiple_of(c * chunk, chunk), chunk)

    def send(c, d, kind, to, own=False):
        return pltpu.make_async_remote_copy(
            src_ref=t_hbm.at[span(c)] if own else tok.at[d, span(c)],
            dst_ref=tok.at[d, span(c)],
            send_sem=ssem.at[c, kind],
            recv_sem=rsem.at[c, d],
            device_id={"head": to},
            device_id_type=MESH,
        )

    def arrived(c, d):
        send(c, d, 0, beside).wait_recv()

    def own_sends(c, act):
        @pl.when(z < last)
        def _():
            act(send(c, place, 0, above, True))
        @pl.when(z > 0)
        def _():
            act(send(c, place, 1, below, True))
        act(send(c, place, 2, beside, True))

    def relays(c, n, e, act):
        d = e * 2 + x
        @pl.when((e > z) & (z > 0))
        def _():
            act(send(c, d, 2 + n, below))
        @pl.when((e < z) & (z < last))
        def _():
            act(send(c, d, 2 + n, above))
        if n == 1:
            @pl.when(c < half)
            def _():
                act(send(c, d, 5 + n, beside))
        else:
            act(send(c, d, 5 + n, beside))

    def twin_sends(act):
        def one(c, carry):
            act(send(c, beside, 9, twin * 2 + x))
            return carry
        lax.fori_loop(half, chunks, one, 0)

    def outputs(c, act, local):
        at = pl.ds(pl.multiple_of(me * rows + c * chunk, chunk), chunk)
        for shift in range(1, size):
            to = lax.rem(me + shift, size)
            act(pltpu.make_async_remote_copy(
                src_ref=stkv.at[c], dst_ref=kv_out.at[at], send_sem=ksend.at[c, shift], recv_sem=krecv.at[c, shift],
                device_id={"seq": to}, device_id_type=MESH))
            act(pltpu.make_async_remote_copy(
                src_ref=stq.at[c, to], dst_ref=q_out.at[at], send_sem=qsend.at[c, shift], recv_sem=qrecv.at[c, shift],
                device_id={"seq": to}, device_id_type=MESH))
        local(pltpu.make_async_copy(stkv.at[c], kv_out.at[at], own_sem.at[c, 0]))
        local(pltpu.make_async_copy(stq.at[c, me], q_out.at[at], own_sem.at[c, 1]))

    start = lambda copy: copy.start()

    def weights_of(d):
        for copy in load(d):
            copy.wait()

    def multiply(row, count, d, first=False):
        at = pl.ds(pl.multiple_of(d * depth, depth), depth)
        to = pl.ds(row, count)
        block = tok[d, to, :]
        for p in range(size):
            cols = slice(p * share, (p + 1) * share)
            v = dot_nn(block, wq[at, cols])
            acc[to, cols] = v if first else acc[to, cols] + v
        v = dot_nn(block, wp[at, :])
        acc[to, width:] = v if first else acc[to, width:] + v

    def each(low, high, body):
        def one(c, carry):
            body(c)
            return carry
        lax.fori_loop(low, high, one, 0)

    each(0, chunks, lambda c: own_sends(c, start))

    def tables(c):
        row = lax.broadcasted_iota(jnp.int32, (chunk, DH), 0) + (me * rows + c * chunk)
        lane = lax.broadcasted_iota(jnp.int32, (chunk, DH), 1)
        angle = row.astype(F32) * frequency_ref[:1, :]
        sine = jnp.sin(angle)
        cos_ref[span(c), :] = jnp.cos(angle)
        sin_ref[span(c), :] = jnp.where(lane < DH // 2, -sine, sine)
    each(0, chunks, tables)
    mine.wait()
    weights_of(place)
    multiply(0, rows, place, True)
    o1, o2, o3 = e1 * 2 + x, e2 * 2 + x, e3 * 2 + x
    f1, f2, f3 = e1 * 2 + 1 - x, e2 * 2 + 1 - x, e3 * 2 + 1 - x

    def column(n, e, d):
        def body(c):
            arrived(c, d)
            relays(c, n, e, start)
        return body
    inner = (z > 0) & (z < last)
    outer = jnp.logical_not(inner)

    def nearest(c):
        column(1, e1, o1)(c)
        @pl.when(inner)
        def _():
            column(2, e2, o2)(c)
    each(0, chunks, nearest)
    weights_of(o1)
    multiply(0, rows, o1)
    each(0, chunks, lambda c: arrived(c, beside))
    @pl.when(outer)
    def _():
        twin_sends(start)
    weights_of(beside)
    multiply(0, rows, beside)
    @pl.when(outer)
    def _():
        each(0, chunks, column(2, e2, o2))
    weights_of(o2)
    multiply(0, rows, o2)
    @pl.when(inner)
    def _():
        each(0, chunks, column(3, e3, o3))
        twin_sends(start)
    each(0, half, lambda c: arrived(c, f1))
    weights_of(f1)
    multiply(0, half * chunk, f1)
    weights_of(o3)
    weights_of(f2)
    weights_of(f3)

    def step(k, carry):
        @pl.when(k < chunks)
        def _():
            @pl.when(outer)
            def _():
                column(3, e3, o3)(k)
            row = pl.multiple_of(k * chunk, chunk)
            multiply(row, chunk, o3)
            arrived(k, f2)
            multiply(row, chunk, f2)
        @pl.when(k >= half)
        def _():
            c = k - half
            row = pl.multiple_of(c * chunk, chunk)
            @pl.when(c >= half)
            def _():
                arrived(c, f1)
                multiply(row, chunk, f1)
            arrived(c, f3)
            multiply(row, chunk, f3)
            cosine = cos_ref[span(c), :]
            sine = sin_ref[span(c), :]
            rotate_rows = lambda v: (v * cosine + pltpu.roll(v, DH // 2, 1) * sine).astype(BF16)
            per = share // DH
            stkv[c, :, :DH] = rotate_rows(acc[span(c), width:width + DH].astype(BF16).astype(F32))
            stkv[c, :, DH:] = acc[span(c), width + DH:].astype(BF16)
            for p in range(size):
                for h in range(per):
                    at = (p * per + h) * DH
                    stq[c, p, :, h * DH:(h + 1) * DH] = rotate_rows(acc[span(c), at:at + DH])
            outputs(c, start, start)
        return carry
    lax.fori_loop(0, chunks + half, step, 0)

    done = lambda copy: copy.wait_send()
    def finish(c):
        own_sends(c, done)
        for n, e in ((1, e1), (2, e2), (3, e3)):
            relays(c, n, e, done)
        outputs(c, lambda copy: copy.wait(), lambda copy: copy.wait())
    each(0, chunks, finish)
    twin_sends(done)

def frequencies():
    exponent = np.arange(DH // 2, dtype=np.float64) * (2.0 / DH)
    table = np.power(ROPE_BASE, -exponent).astype(np.float32)
    return jnp.asarray(np.tile(np.concatenate([table, table])[None], (8, 1)))


def project_exchange(tokens, w_query, w_key, w_value, chunks=8):
    size = lax.axis_size("seq")
    rows, depth = tokens.shape
    full, width = w_query.shape
    share = width // size
    chunk = rows // chunks
    blocks = full // depth
    any_ = pl.BlockSpec(memory_space=pl.ANY)
    vm = pl.BlockSpec(memory_space=pltpu.VMEM)
    dma = pltpu.SemaphoreType.DMA
    return pl.pallas_call(
        functools.partial(project_kernel, chunk),
        out_shape=(jax.ShapeDtypeStruct((rows * size, share), BF16), jax.ShapeDtypeStruct((rows * size, 2 * DH), BF16)),
        in_specs=[any_] * 4 + [vm],
        out_specs=(any_, any_),
        scratch_shapes=[
            pltpu.VMEM((rows, DH), F32),
            pltpu.VMEM((rows, DH), F32),
            pltpu.VMEM((blocks, rows, depth), BF16),
            pltpu.VMEM((full, width), BF16),
            pltpu.VMEM((full, 2 * DH), BF16),
            pltpu.VMEM((rows, width + 2 * DH), F32),
            pltpu.VMEM((chunks, size, chunk, share), BF16),
            pltpu.VMEM((chunks, chunk, 2 * DH), BF16),
            dma((chunks, 10)), dma((chunks, blocks)), dma((3, blocks)), dma,
            dma((chunks, size)), dma((chunks, size)), dma((chunks, size)), dma((chunks, size)), dma((chunks, 2)),
        ],
        compiler_params=pltpu.CompilerParams(collective_id=0, has_side_effects=True, vmem_limit_bytes=48 * 2**20),
        cost_estimate=pl.CostEstimate(flops=2 * rows * full * (width + 2 * DH), bytes_accessed=full * width * 2, transcendentals=0),
    )(tokens, w_query, w_key, w_value, frequencies())


def per_device_by_heads(tokens, w_query, w_key, w_value, map_query, map_key):
    row_count = tokens.shape[0]
    queries, pair = project_exchange(tokens, w_query, w_key, w_value)
    return attention(queries, pair, map_query, map_key, row_count)


def fits(mesh, tokens, w_query, w_key):
    heads = w_query.shape[1] // mesh.shape["head"] // DH
    rows = tokens.shape[0] // mesh.shape["seq"]
    return (
        mesh.shape["head"] == 8
        and w_key.shape[1] // mesh.shape["head"] == DH
        and heads % mesh.shape["seq"] == 0
        and rows % 256 == 0
    )


def solution(mesh):
    in_specs = (
        P("seq", "head"),
        P(None, "head"),
        P(None, "head"),
        P(None, "head"),
        P("head", None, None),
        P("head", None, None),
    )
    out_specs = (P("seq", "head"), P("head", None, None), P("head", None, None))

    def run(tokens, w_query, w_key, w_value, map_query, map_key):
        body = per_device_by_heads if fits(mesh, tokens, w_query, w_key) else per_device_by_rows
        return jax.shard_map(
            body, mesh=mesh, in_specs=in_specs, out_specs=out_specs, check_vma=False
        )(tokens, w_query, w_key, w_value, map_query, map_key)

    return run
```
